512 devices in a mesh: dp: 32 (over y, x), mp: 16 (over z, core).
Axes of the slice: x: 4, y: 8, z: 8, core: 2. Of those that a mesh axis runs over, the one named last changes fastest.
Arguments:
- query_new: bfloat16 [512, 4096], P(('dp', 'mp')), parts along dimension 0, may hold values from -140 to 140
- key_new: bfloat16 [512, 1024], P(('dp', 'mp')), parts along dimension 0, may hold values from -5 to 5
- value_new: bfloat16 [512, 1024], P(('dp', 'mp')), parts along dimension 0, may hold values from -5 to 5
- prefix_keys: bfloat16 [65536, 1024], P(('dp', 'mp')), parts along dimension 0, may hold values from -5 to 5
- prefix_values: bfloat16 [65536, 1024], P(('dp', 'mp')), parts along dimension 0, may hold values from -5 to 5
- sample_suffix_keys: bfloat16 [512, 64, 1024], P(('dp', 'mp')), parts along dimension 0, may hold values from -5 to 5
- sample_suffix_values: bfloat16 [512, 64, 1024], P(('dp', 'mp')), parts along dimension 0, may hold values from -5 to 5
- prefix_len: int32 [32], P('dp'), parts along dimension 0, may hold values from 512 to 2048
- suffix_len: int32 [512], P(('dp', 'mp')), parts along dimension 0, may hold values from 1 to 64, as said below
- residual: bfloat16 [512, 8192], P(('dp', 'mp')), parts along dimension 0, may hold values from -3 to 3
- out_weight: bfloat16 [4096, 8192], P('mp'), may hold values from -0.1875 to 0.1875
- norm_gain: bfloat16 [8192], replicated, may hold values from 0.5 to 1.5
Outputs:
- hidden: bfloat16 [512, 8192], P(('dp', 'mp')), parts along dimension 0
- normed: bfloat16 [512, 8192], P(('dp', 'mp')), parts along dimension 0
The draws below stay inside these ranges and needn't reach their ends.
There are 32 independent parts, one for each index of `dp`. The reference program is written for one: setup_inputs(seed, part) draws one part's arguments, and reference() takes and returns one part's arrays. A program takes and returns all parts, laid end to end along the dimension named above; an argument that names none is the same for every part. Nothing has to cross between parts.
Inputs may be any that keep to these rules, and one draw needn't show every extreme that they name: `suffix_len`: some sample has exactly 64 cached generated tokens.
All inputs are finite; a program needn't handle non-finite values.
Results may differ from the reference program's by a relative error of at most 0.0085.
Values may be sent and summed in bfloat16 or wider, within the bound.
A program may use at most 64 MiB of HBM per device.

```python
import jax
import jax.numpy as jnp
from jax import lax

D = 8192
HEAD_SIZE = 128
KEY_VALUE_HEADS = 8
HQ = 32
SUFFIX_POSITIONS = 64
SAMPLE_COUNT = 16
PRE = 2048


def joint_keys_queries(key):
    base = jax.random.fold_in(key, 7)
    keys = jnp.clip(jax.random.normal(jax.random.fold_in(base, 1), (PRE, KEY_VALUE_HEADS * HEAD_SIZE), jnp.float32), -5.0, 5.0)
    queries = jnp.clip(2.0 * jax.random.normal(jax.random.fold_in(base, 2), (SAMPLE_COUNT, HQ * HEAD_SIZE), jnp.float32), -8.0, 8.0)
    return (keys, queries)


def draw_prefix_keys(key, part):
    keys, queries = joint_keys_queries(key)
    return keys.astype(jnp.bfloat16)


def draw_query_new(key, part):
    keys, queries = joint_keys_queries(key)
    return queries.astype(jnp.bfloat16)


def draw_suffix_len(key, part):
    base = jax.random.fold_in(key, 31)
    lengths = jax.random.randint(jax.random.fold_in(base, 1), (SAMPLE_COUNT,), 1, SUFFIX_POSITIONS + 1, dtype=jnp.int32)
    chosen = jax.random.randint(jax.random.fold_in(base, 2), (), 0, SAMPLE_COUNT, dtype=jnp.int32)
    lengths = jnp.where(jnp.arange(SAMPLE_COUNT, dtype=jnp.int32) == chosen, SUFFIX_POSITIONS, lengths)
    return lengths.astype(jnp.int32)


def block_levels(stream_key, shape, pieces, low, top_value):
    factor_of, own = 1.0, jax.random.fold_in(stream_key, 6)
    for axis_at, blocks in pieces:
        heights = jnp.exp(jax.random.uniform(jax.random.fold_in(own, axis_at), (blocks,), jnp.float32, low / len(pieces), top_value / len(pieces)))
        factor_of = factor_of * jnp.repeat(heights, shape[axis_at] // blocks).reshape([-1 if axis == axis_at else 1 for axis in range(len(shape))])
    return factor_of


def centred(own_key, shape, deviation, limit, split=(), kind=jnp.bfloat16):
    array = jax.random.normal(own_key, shape, jnp.float32) * deviation
    if len(split) > 0:
        array = block_levels(own_key, shape, split, -0.22, 0.18) * array
    return jnp.clip(array, min=-limit, max=limit).astype(kind)


def setup_inputs(seed: int = 0, part: int = 0) -> dict:
    arg_keys = jax.random.split(jax.random.key(seed), 13)
    part_keys = jax.random.split(jax.random.fold_in(arg_keys[12], part), 13)
    return {
        "query_new": draw_query_new(jax.random.fold_in(jax.random.fold_in(arg_keys[12], part), 71), part),
        "key_new": centred(part_keys[1], (SAMPLE_COUNT, KEY_VALUE_HEADS * HEAD_SIZE), 1.0, 5.0, ((0, 16),)),
        "value_new": centred(part_keys[2], (SAMPLE_COUNT, KEY_VALUE_HEADS * HEAD_SIZE), 1.0, 5.0, ((0, 16),)),
        "prefix_keys": draw_prefix_keys(jax.random.fold_in(jax.random.fold_in(arg_keys[12], part), 71), part),
        "prefix_values": centred(part_keys[4], (PRE, KEY_VALUE_HEADS * HEAD_SIZE), 1.0, 5.0, ((0, 16),)),
        "sample_suffix_keys": centred(part_keys[5], (SAMPLE_COUNT, SUFFIX_POSITIONS, KEY_VALUE_HEADS * HEAD_SIZE), 1.0, 5.0, ((0, 16),)),
        "sample_suffix_values": centred(part_keys[6], (SAMPLE_COUNT, SUFFIX_POSITIONS, KEY_VALUE_HEADS * HEAD_SIZE), 1.0, 5.0, ((0, 16),)),
        "prefix_len": jax.random.randint(part_keys[7], (1,), PRE // 4, PRE + 1).astype(jnp.int32),
        "suffix_len": draw_suffix_len(jax.random.fold_in(jax.random.fold_in(arg_keys[12], part), 71), part),
        "residual": centred(part_keys[9], (SAMPLE_COUNT, D), 0.5, 3.0, ((0, 16),)),
        "out_weight": centred(arg_keys[10], (HQ * HEAD_SIZE, D), (HQ * HEAD_SIZE // 4) ** -0.5, 0.1875, ((0, 16),)),
        "norm_gain": jnp.clip(1.0 + 0.1 * jax.random.normal(arg_keys[11], (D,), jnp.float32), 0.5, 1.5).astype(jnp.bfloat16),
    }


def reference(query_new, key_new, value_new, prefix_keys, prefix_values, sample_suffix_keys, sample_suffix_values, prefix_len, suffix_len, residual, out_weight, norm_gain):
    group = HQ // KEY_VALUE_HEADS
    score_scale = HEAD_SIZE ** (-0.5)
    query_vector = query_new.astype(jnp.float32).reshape(SAMPLE_COUNT, KEY_VALUE_HEADS, group, HEAD_SIZE)
    pkeys = prefix_keys.astype(jnp.float32).reshape(PRE, KEY_VALUE_HEADS, HEAD_SIZE)
    prefix_value_rows = prefix_values.astype(jnp.float32).reshape(PRE, KEY_VALUE_HEADS, HEAD_SIZE)
    suffix_key_rows = sample_suffix_keys.astype(jnp.float32).reshape(SAMPLE_COUNT, SUFFIX_POSITIONS, KEY_VALUE_HEADS, HEAD_SIZE)
    suffix_value_rows = sample_suffix_values.astype(jnp.float32).reshape(SAMPLE_COUNT, SUFFIX_POSITIONS, KEY_VALUE_HEADS, HEAD_SIZE)
    fresh_key_rows = key_new.astype(jnp.float32).reshape(SAMPLE_COUNT, KEY_VALUE_HEADS, HEAD_SIZE)
    nvals = value_new.astype(jnp.float32).reshape(SAMPLE_COUNT, KEY_VALUE_HEADS, HEAD_SIZE)
    pvalid = jnp.arange(PRE, dtype=jnp.int32) < prefix_len[0]
    svalid = jnp.arange(SUFFIX_POSITIONS, dtype=jnp.int32)[None, :] < suffix_len[:, None]
    s_pre = jnp.einsum('bkgd,pkd->bkgp', query_vector, pkeys) * score_scale
    suffix_score_rows = jnp.einsum('cqxt,caqt->cqxa', query_vector, suffix_key_rows) * score_scale
    fresh_score_rows = jnp.einsum('exio,exo->exi', query_vector, fresh_key_rows) * score_scale
    s_pre = jnp.where(pvalid[None, None, None, :], s_pre, -jnp.inf)
    suffix_score_rows = jnp.where(svalid[:, None, None, :], suffix_score_rows, -jnp.inf)
    top = jnp.maximum(jnp.maximum(lax.optimization_barrier(jnp.max(s_pre, -1)), lax.optimization_barrier(jnp.max(suffix_score_rows, -1))), fresh_score_rows)
    w_pre = jnp.exp(s_pre - top[..., None])
    suffix_weight_rows = jnp.exp(suffix_score_rows - top[..., None])
    w_new = jnp.exp(fresh_score_rows - top)
    total = lax.optimization_barrier(jnp.sum(w_pre, -1)) + lax.optimization_barrier(jnp.sum(suffix_weight_rows, -1)) + w_new
    prefix_bias_rows = w_pre.astype(jnp.bfloat16).astype(jnp.float32)
    suffix_bias_rows = suffix_weight_rows.astype(jnp.bfloat16).astype(jnp.float32)
    b_new = w_new.astype(jnp.bfloat16).astype(jnp.float32)
    summed_rows = jnp.einsum('wnso,onr->wnsr', prefix_bias_rows, prefix_value_rows) + jnp.einsum('cjax,cxjq->cjaq', suffix_bias_rows, suffix_value_rows)
    summed_rows = summed_rows + b_new[..., None] * nvals[:, :, None, :]
    attn = (summed_rows / total[..., None]).astype(jnp.bfloat16).reshape(SAMPLE_COUNT, HQ * HEAD_SIZE)
    proj = jnp.dot(attn, out_weight, preferred_element_type=jnp.float32)
    stream = residual.astype(jnp.float32) + proj
    hidden = stream.astype(jnp.bfloat16)
    meansq = lax.optimization_barrier(jnp.mean(stream * stream, axis=-1, keepdims=True))
    normed = (stream * jax.lax.rsqrt(meansq + 1e-05) * norm_gain.astype(jnp.float32)[None, :]).astype(jnp.bfloat16)
    return (hidden, normed)
```

```python
import functools

import jax
import jax.numpy as jnp
from jax import lax
from jax.experimental import pallas as pl
from jax.experimental.pallas import tpu as pltpu
from jax.sharding import PartitionSpec as P

HEAD = 128
KVH = 8
HQ = 32
D = 8192
CHIPS = 8
N = 16
HALF_HEADS = 16
HALF_KV = 4
PRE_DEV = 128
SUF = 64
BLOCK = 256
HALF_COLS = HALF_KV * HEAD
HALF_D = D // 2
GROUPS = 2
GROUP_COLS = HALF_D // GROUPS
NEG = -1e30
F32 = jnp.float32
BF16 = jnp.bfloat16
ORDER = (4, 3, 5, 2, 6, 1, 7)


def nt(a, b):
    return lax.dot_general(a, b, (((1,), (1,)), ((), ())), preferred_element_type=F32)


def nn(a, b):
    return lax.dot_general(a, b, (((1,), (0,)), ((), ())), preferred_element_type=F32)


def kernel(
    q_hbm,
    kn_hbm,
    vn_hbm,
    pk_hbm,
    pv_hbm,
    sk_hbm,
    sv_hbm,
    plen_ref,
    slen_ref,
    res_hbm,
    w_hbm,
    gain_hbm,
    hid_ref,
    nrm_ref,
    qv,
    knv,
    vnv,
    resv,
    gainv,
    kfull,
    vfull,
    kpar,
    vpar,
    bias,
    bpar,
    q32,
    qsend,
    qbuf,
    perm,
    ostage,
    sstage,
    obuf,
    sbuf,
    abuf,
    wbuf,
    ysend,
    rbuf,
    res64,
    gain64,
    loc_sem,
    qs_sem,
    qr_sem,
    xs_sem,
    xr_sem,
    os_sem,
    or_sem,
    ss_sem,
    sr_sem,
    ys_sem,
    yr_sem,
):
    me = lax.axis_index("mp")
    z = me // 2
    c = me % 2
    p = 1 - c
    partner = z * 2 + p

    def at_mp(index):
        return {"mp": index}

    def remote(src, dst, ssem, rsem, index):
        return pltpu.make_async_remote_copy(
            src_ref=src,
            dst_ref=dst,
            send_sem=ssem,
            recv_sem=rsem,
            device_id=at_mp(index),
            device_id_type=pl.DeviceIdType.MESH,
        )

    barrier = pltpu.get_barrier_semaphore()
    for step in range(1, N):
        pl.semaphore_signal(
            barrier,
            inc=1,
            device_id=at_mp((me + step) % N),
            device_id_type=pl.DeviceIdType.MESH,
        )

    own_cols = pl.ds(pl.multiple_of(c * HALF_COLS, HALF_COLS), HALF_COLS)
    par_cols = pl.ds(pl.multiple_of(p * HALF_COLS, HALF_COLS), HALF_COLS)
    own_d = pl.ds(pl.multiple_of(c * HALF_D, HALF_D), HALF_D)
    par_d = pl.ds(pl.multiple_of(p * HALF_D, HALF_D), HALF_D)

    local = [
        pltpu.make_async_copy(q_hbm, qv, loc_sem.at[0]),
        pltpu.make_async_copy(kn_hbm, knv, loc_sem.at[1]),
        pltpu.make_async_copy(vn_hbm, vnv, loc_sem.at[2]),
        pltpu.make_async_copy(pk_hbm, kfull.at[pl.ds(0, PRE_DEV)], loc_sem.at[3]),
        pltpu.make_async_copy(pv_hbm, vfull.at[pl.ds(0, PRE_DEV)], loc_sem.at[4]),
        pltpu.make_async_copy(sk_hbm.at[0], kfull.at[pl.ds(PRE_DEV, SUF)], loc_sem.at[5]),
        pltpu.make_async_copy(sv_hbm.at[0], vfull.at[pl.ds(PRE_DEV, SUF)], loc_sem.at[6]),
        pltpu.make_async_copy(res_hbm, resv, loc_sem.at[7]),
        pltpu.make_async_copy(gain_hbm, gainv, loc_sem.at[8]),
        pltpu.make_async_copy(w_hbm.at[:, own_d], wbuf.at[c], loc_sem.at[9]),
    ]
    for copy in local:
        copy.start()

    rows = lax.broadcasted_iota(jnp.int32, (BLOCK, BLOCK), 0)
    cols = lax.broadcasted_iota(jnp.int32, (BLOCK, BLOCK), 1)
    perm[...] = jnp.where(cols == (rows % N) * N + rows // N, 1.0, 0.0).astype(BF16)
    col = lax.broadcasted_iota(jnp.int32, (8, BLOCK), 1)
    valid = (
        ((col < PRE_DEV) & (col + me * PRE_DEV < plen_ref[0]))
        | ((col >= PRE_DEV) & (col < PRE_DEV + SUF) & (col - PRE_DEV < slen_ref[0]))
        | (col == PRE_DEV + SUF)
    )
    bias[...] = jnp.where(valid, 0.0, NEG)

    local[0].wait()
    for h in range(HQ):
        q32[h : h + 1, :] = qv[0:1, h * HEAD : (h + 1) * HEAD].astype(F32)
    qsend[0] = q32[0:HALF_HEADS, :].astype(BF16)
    qsend[1] = q32[HALF_HEADS:HQ, :].astype(BF16)
    qbuf[me] = qsend[c]

    pad_rows = BLOCK - PRE_DEV - SUF
    first = lax.broadcasted_iota(jnp.int32, (pad_rows, KVH * HEAD), 0) == 0
    local[1].wait()
    kfull[PRE_DEV + SUF : BLOCK, :] = jnp.where(first, knv[0:1, :].astype(F32), 0.0).astype(BF16)
    local[2].wait()
    vfull[PRE_DEV + SUF : BLOCK, :] = jnp.where(first, vnv[0:1, :].astype(F32), 0.0).astype(BF16)

    pl.semaphore_wait(barrier, N - 1)

    sends = []
    for step in ORDER:
        for half in range(2):
            target = ((z + step) % CHIPS) * 2 + half
            copy = remote(
                qsend.at[half], qbuf.at[me], qs_sem.at[step * 2 + half], qr_sem.at[me], target
            )
            copy.start()
            sends.append(copy)
    copy = remote(qsend.at[p], qbuf.at[me], qs_sem.at[0], qr_sem.at[me], partner)
    copy.start()
    sends.append(copy)

    for copy in local[3:7]:
        copy.wait()
    swaps = [
        remote(kfull.at[:, par_cols], kpar, xs_sem.at[0], xr_sem.at[0], partner),
        remote(vfull.at[:, par_cols], vpar, xs_sem.at[1], xr_sem.at[1], partner),
        remote(bias, bpar, xs_sem.at[2], xr_sem.at[2], partner),
        remote(w_hbm.at[:, par_d], wbuf.at[c], xs_sem.at[3], xr_sem.at[3], partner),
    ]
    for copy in swaps:
        copy.start()

    local[7].wait()
    local[8].wait()
    for r in range(D // HEAD):
        res64[r : r + 1, :] = resv[0:1, r * HEAD : (r + 1) * HEAD].astype(F32)
        gain64[r : r + 1, :] = gainv[0:1, r * HEAD : (r + 1) * HEAD].astype(F32)

    for copy in swaps[0:3]:
        copy.wait_recv()
    for step in range(1, N):
        source = (me + step) % N
        remote(qsend.at[0], qbuf.at[source], qs_sem.at[0], qr_sem.at[source], source).wait_recv()

    queries = nn(perm[...], qbuf[...].reshape(N * HALF_HEADS, HEAD)).astype(BF16)
    row64 = lax.broadcasted_iota(jnp.int32, (64, BLOCK), 0) % N
    col64 = lax.broadcasted_iota(jnp.int32, (64, BLOCK), 1)
    shown_own = (col64 < PRE_DEV) | (row64 == me)
    shown_par = (col64 < PRE_DEV) | (row64 == partner)
    lane16 = lax.broadcasted_iota(jnp.int32, (N, HEAD), 1) % N
    sub16 = lax.broadcasted_iota(jnp.int32, (N, HEAD), 0)
    diagonal = lane16 == sub16
    scale = HEAD ** (-0.5)
    bias_own = bias[0:1, :]
    bias_par = bpar[0:1, :]
    for j in range(HALF_KV):
        qj = queries[64 * j : 64 * (j + 1), :]
        own_j = pl.ds(pl.multiple_of(c * HALF_COLS + j * HEAD, HEAD), HEAD)
        s_own = nt(qj, kfull[:, own_j]) * scale + bias_own
        s_par = nt(qj, kpar[:, j * HEAD : (j + 1) * HEAD]) * scale + bias_par
        s_own = jnp.where(shown_own, s_own, NEG)
        s_par = jnp.where(shown_par, s_par, NEG)
        top = jnp.max(jnp.maximum(s_own, s_par), axis=1, keepdims=True)
        w_own = jnp.exp(s_own - top)
        w_par = jnp.exp(s_par - top)
        total = jnp.sum(w_own + w_par, axis=1, keepdims=True)
        out = nn(w_own.astype(BF16), vfull[:, own_j]) + nn(
            w_par.astype(BF16), vpar[:, j * HEAD : (j + 1) * HEAD]
        )
        for hh in range(4):
            part = slice(N * hh, N * (hh + 1))
            ostage[4 * j + hh] = out[part, :].astype(BF16)
            tops = jnp.sum(jnp.where(diagonal, top[part, :], 0.0), axis=0, keepdims=True)
            totals = jnp.sum(jnp.where(diagonal, total[part, :], 0.0), axis=0, keepdims=True)
            g = 2 * j + hh // 2
            sstage[g, hh % 2 : hh % 2 + 1, :] = tops
            sstage[g, 2 + hh % 2 : 3 + hh % 2, :] = totals
        for d in range(2):
            g = 2 * j + d
            target = (4 * c + j) * 2 + d
            for src, dst, ssem, rsem in (
                (ostage.at[pl.ds(2 * g, 2)], obuf.at[:, z], os_sem.at[g], or_sem.at[z]),
                (sstage.at[g], sbuf.at[z], ss_sem.at[g], sr_sem.at[z]),
            ):

                @pl.when(target != me)
                def _():
                    remote(src, dst, ssem, rsem, target).start()

                @pl.when(target == me)
                def _():
                    pltpu.make_async_copy(src, dst, rsem).start()

    for src_z in range(CHIPS):
        pltpu.make_async_copy(obuf.at[:, src_z], obuf.at[:, src_z], or_sem.at[src_z]).wait()
        pltpu.make_async_copy(sbuf.at[src_z], sbuf.at[src_z], sr_sem.at[src_z]).wait()
    stats = sbuf[...]
    group = lax.broadcasted_iota(jnp.int32, (2, HEAD), 1) // N
    most = stats[0, 0:2, :]
    for src_z in range(1, CHIPS):
        most = jnp.maximum(most, stats[src_z, 0:2, :])
    summed = jnp.zeros((2, HEAD), F32)
    factor = jnp.zeros((2, HEAD), F32)
    for src_z in range(CHIPS):
        f = jnp.exp(stats[src_z, 0:2, :] - most)
        summed = summed + f * stats[src_z, 2:4, :]
        factor = jnp.where(group == src_z, f, factor)
    factor = factor / summed
    for hh in range(2):
        mix = jnp.where(diagonal, factor[hh : hh + 1, :], 0.0)
        high = mix.astype(BF16)
        low = (mix - high.astype(F32)).astype(BF16)
        rows_h = obuf[hh].reshape(CHIPS * N, HEAD)
        abuf[c, :, hh * HEAD : (hh + 1) * HEAD] = (nn(high, rows_h) + nn(low, rows_h)).astype(BF16)
    attn_swap = remote(abuf.at[c], abuf.at[c], xs_sem.at[4], xr_sem.at[4], partner)
    attn_swap.start()

    local[9].wait()
    swaps[3].wait_recv()
    attn_swap.wait_recv()
    for group_at in range(GROUPS):
        at = slice(group_at * GROUP_COLS, (group_at + 1) * GROUP_COLS)
        y = nn(abuf[0], wbuf[0, :, at]) + nn(abuf[1], wbuf[1, :, at])
        y = y.astype(BF16)
        y = jnp.concatenate([y[:, HEAD * i : HEAD * (i + 1)] for i in range(N)], axis=0)
        y = nn(perm[...], y).astype(BF16)
        ysend[group_at] = y.reshape(N, N, HEAD)
        for step in ORDER:
            for half in range(2):
                target = ((z + step) % CHIPS) * 2 + half
                at_sem = group_at * N + step * 2 + half
                copy = remote(
                    ysend.at[group_at, target],
                    rbuf.at[z, c, group_at],
                    ys_sem.at[at_sem],
                    yr_sem.at[z, c, group_at],
                    target,
                )
                copy.start()
                sends.append(copy)
        copy = remote(
            ysend.at[group_at, partner],
            rbuf.at[z, c, group_at],
            ys_sem.at[group_at * N],
            yr_sem.at[z, c, group_at],
            partner,
        )
        copy.start()
        sends.append(copy)
        rbuf[z, c, group_at] = ysend[group_at, me]

    for step in range(1, N):
        source = (me + step) % N
        for group_at in range(GROUPS):
            at = rbuf.at[source // 2, source % 2, group_at]
            pltpu.make_async_copy(at, at, yr_sem.at[source // 2, source % 2, group_at]).wait()
    stream = res64[...] + jnp.sum(rbuf[...].astype(F32), axis=0).reshape(D // HEAD, HEAD)
    meansq = jnp.sum(stream * stream, keepdims=True) * (1.0 / D)
    normed = stream * lax.rsqrt(meansq + 1e-05) * gain64[...]
    hid_ref[...] = stream.astype(BF16)
    nrm_ref[...] = normed.astype(BF16)

    for copy in sends:
        copy.wait_send()
    for copy in swaps:
        copy.wait_send()
    attn_swap.wait_send()
    for j in range(HALF_KV):
        for d in range(2):
            g = 2 * j + d
            target = (4 * c + j) * 2 + d

            @pl.when(target != me)
            def _():
                remote(
                    ostage.at[pl.ds(2 * g, 2)], obuf.at[:, z], os_sem.at[g], or_sem.at[z], target
                ).wait_send()
                remote(
                    sstage.at[g], sbuf.at[z], ss_sem.at[g], sr_sem.at[z], target
                ).wait_send()


def local(
    query_new,
    key_new,
    value_new,
    prefix_keys,
    prefix_values,
    sample_suffix_keys,
    sample_suffix_values,
    prefix_len,
    suffix_len,
    residual,
    out_weight,
    norm_gain,
):
    hbm = pl.BlockSpec(memory_space=pl.ANY)
    smem = pl.BlockSpec(memory_space=pltpu.SMEM)
    vmem = pl.BlockSpec(memory_space=pltpu.VMEM)
    dma = pltpu.SemaphoreType.DMA
    hidden, normed = pl.pallas_call(
        kernel,
        out_shape=(
            jax.ShapeDtypeStruct((D // HEAD, HEAD), BF16),
            jax.ShapeDtypeStruct((D // HEAD, HEAD), BF16),
        ),
        in_specs=[hbm] * 7 + [smem] * 2 + [hbm] * 3,
        out_specs=(vmem, vmem),
        scratch_shapes=[
            pltpu.VMEM((1, HQ * HEAD), BF16),
            pltpu.VMEM((1, KVH * HEAD), BF16),
            pltpu.VMEM((1, KVH * HEAD), BF16),
            pltpu.VMEM((1, D), BF16),
            pltpu.VMEM((1, D), BF16),
            pltpu.VMEM((BLOCK, KVH * HEAD), BF16),
            pltpu.VMEM((BLOCK, KVH * HEAD), BF16),
            pltpu.VMEM((BLOCK, HALF_COLS), BF16),
            pltpu.VMEM((BLOCK, HALF_COLS), BF16),
            pltpu.VMEM((8, BLOCK), F32),
            pltpu.VMEM((8, BLOCK), F32),
            pltpu.VMEM((HQ, HEAD), F32),
            pltpu.VMEM((2, HALF_HEADS, HEAD), BF16),
            pltpu.VMEM((N, HALF_HEADS, HEAD), BF16),
            pltpu.VMEM((BLOCK, BLOCK), BF16),
            pltpu.VMEM((HALF_HEADS, N, HEAD), BF16),
            pltpu.VMEM((CHIPS, 4, HEAD), F32),
            pltpu.VMEM((2, CHIPS, N, HEAD), BF16),
            pltpu.VMEM((CHIPS, 4, HEAD), F32),
            pltpu.VMEM((2, N, 2 * HEAD), BF16),
            pltpu.VMEM((2, 2 * HEAD, HALF_D), BF16),
            pltpu.VMEM((GROUPS, N, N, HEAD), BF16),
            pltpu.VMEM((CHIPS, 2, GROUPS, N, HEAD), BF16),
            pltpu.VMEM((D // HEAD, HEAD), F32),
            pltpu.VMEM((D // HEAD, HEAD), F32),
            dma((10,)),
            dma((N,)),
            dma((N,)),
            dma((5,)),
            dma((5,)),
            dma((CHIPS,)),
            dma((CHIPS,)),
            dma((CHIPS,)),
            dma((CHIPS,)),
            dma((GROUPS * N,)),
            dma((CHIPS, 2, GROUPS)),
        ],
        compiler_params=pltpu.CompilerParams(collective_id=0, has_side_effects=True),
        name="decode_step",
    )(
        query_new,
        key_new,
        value_new,
        prefix_keys,
        prefix_values,
        sample_suffix_keys,
        sample_suffix_values,
        prefix_len,
        suffix_len,
        residual,
        out_weight,
        norm_gain.reshape(1, D),
    )
    return hidden.reshape(1, D), normed.reshape(1, D)


def solution(mesh):
    placed = (
        P(("dp", "mp"), None),
        P(("dp", "mp"), None),
        P(("dp", "mp"), None),
        P(("dp", "mp"), None),
        P(("dp", "mp"), None),
        P(("dp", "mp"), None, None),
        P(("dp", "mp"), None, None),
        P("dp"),
        P(("dp", "mp")),
        P(("dp", "mp"), None),
        P("mp", None),
        P(),
    )
    return jax.shard_map(
        local,
        mesh=mesh,
        in_specs=placed,
        out_specs=(P(("dp", "mp"), None), P(("dp", "mp"), None)),
        check_vma=False,
    )
```

```python
import functools

import jax
import jax.numpy as jnp
from jax import lax
from jax.experimental import pallas as pl
from jax.experimental.pallas import tpu as pltpu
from jax.sharding import PartitionSpec as P

HEAD = 128
KVH = 8
HQ = 32
D = 8192
CHIPS = 8
N = 16
HALF_HEADS = 16
HALF_KV = 4
PRE_DEV = 128
SUF = 64
BLOCK = 256
HALF_COLS = HALF_KV * HEAD
HALF_D = D // 2
GROUPS = 2
GROUP_COLS = HALF_D // GROUPS
NEG = -1e30
F32 = jnp.float32
BF16 = jnp.bfloat16
HALF_CHIPS = CHIPS // 2
SB = N // 2
RB = 4 * SB


def nt(a, b):
    return lax.dot_general(a, b, (((1,), (1,)), ((), ())), preferred_element_type=F32)


def nn(a, b):
    return lax.dot_general(a, b, (((1,), (0,)), ((), ())), preferred_element_type=F32)


def kernel(
    q_hbm,
    kn_hbm,
    vn_hbm,
    pk_hbm,
    pv_hbm,
    sk_hbm,
    sv_hbm,
    plen_hbm,
    slen_hbm,
    res_hbm,
    w_hbm,
    gain_hbm,
    hid_ref,
    nrm_ref,
    qv,
    knv,
    vnv,
    resv,
    gainv,
    kfull,
    vfull,
    kpar,
    vpar,
    bias,
    bpar,
    q32,
    qsend,
    qbuf,
    to_heads,
    to_samples,
    ostage,
    sstage,
    obuf,
    sbuf,
    wbuf,
    ysend,
    rbuf,
    res64,
    gain64,
    plen_ref,
    slen_ref,
    loc_sem,
    qs_sem,
    qr_sem,
    xs_sem,
    xr_sem,
    os_sem,
    or_sem,
    ss_sem,
    sr_sem,
    ys_sem,
    yr_sem,
):
    me = lax.axis_index("mp")
    z = me // 2
    c = me % 2
    p = 1 - c
    partner = z * 2 + p
    my_batch = z // HALF_CHIPS

    def at_mp(index):
        return {"mp": index}

    def remote(src, dst, ssem, rsem, index):
        return pltpu.make_async_remote_copy(
            src_ref=src,
            dst_ref=dst,
            send_sem=ssem,
            recv_sem=rsem,
            device_id=at_mp(index),
            device_id_type=pl.DeviceIdType.MESH,
        )

    def wait_bytes(ref, sem):
        pltpu.make_async_copy(ref, ref, sem).wait()

    own_cols = pl.ds(pl.multiple_of(c * HALF_COLS, HALF_COLS), HALF_COLS)
    par_cols = pl.ds(pl.multiple_of(p * HALF_COLS, HALF_COLS), HALF_COLS)
    own_d = pl.ds(pl.multiple_of(c * HALF_D, HALF_D), HALF_D)
    par_d = pl.ds(pl.multiple_of(p * HALF_D, HALF_D), HALF_D)
    swaps = [
        remote(kfull.at[:, par_cols], kpar, xs_sem.at[0], xr_sem.at[0], partner),
        remote(vfull.at[:, par_cols], vpar, xs_sem.at[1], xr_sem.at[1], partner),
        remote(bias, bpar, xs_sem.at[2], xr_sem.at[2], partner),
        remote(w_hbm.at[:, par_d], wbuf.at[c], xs_sem.at[3], xr_sem.at[3], partner),
    ]
    local = [
        pltpu.make_async_copy(q_hbm, qv, loc_sem.at[0]),
        pltpu.make_async_copy(kn_hbm, knv, loc_sem.at[1]),
        pltpu.make_async_copy(vn_hbm, vnv, loc_sem.at[2]),
        pltpu.make_async_copy(pk_hbm, kfull.at[pl.ds(0, PRE_DEV)], loc_sem.at[3]),
        pltpu.make_async_copy(pv_hbm, vfull.at[pl.ds(0, PRE_DEV)], loc_sem.at[4]),
        pltpu.make_async_copy(sk_hbm.at[0], kfull.at[pl.ds(PRE_DEV, SUF)], loc_sem.at[5]),
        pltpu.make_async_copy(sv_hbm.at[0], vfull.at[pl.ds(PRE_DEV, SUF)], loc_sem.at[6]),
        pltpu.make_async_copy(res_hbm, resv, loc_sem.at[7]),
        pltpu.make_async_copy(gain_hbm, gainv, loc_sem.at[8]),
        pltpu.make_async_copy(w_hbm.at[:, own_d], wbuf.at[c], loc_sem.at[9]),
        pltpu.make_async_copy(plen_hbm, plen_ref, loc_sem.at[10]),
        pltpu.make_async_copy(slen_hbm, slen_ref, loc_sem.at[11]),
    ]

    with jax.named_scope("prep"):
        barrier = pltpu.get_barrier_semaphore()

        def greet(step, carry):
            pl.semaphore_signal(
                barrier,
                inc=1,
                device_id=at_mp((me + step) % N),
                device_id_type=pl.DeviceIdType.MESH,
            )
            return carry

        lax.fori_loop(1, N, greet, 0)
        for copy in local:
            copy.start()

        rows = lax.broadcasted_iota(jnp.int32, (HEAD, HEAD), 0)
        cols = lax.broadcasted_iota(jnp.int32, (HEAD, HEAD), 1)
        to_heads[...] = jnp.where(cols == (rows % SB) * N + rows // SB, 1.0, 0.0).astype(BF16)
        to_samples[...] = jnp.where(cols == (rows % N) * SB + rows // N, 1.0, 0.0).astype(BF16)
        local[10].wait()
        local[11].wait()
        col = lax.broadcasted_iota(jnp.int32, (8, BLOCK), 1)
        valid = (
            ((col < PRE_DEV) & (col + me * PRE_DEV < plen_ref[0]))
            | ((col >= PRE_DEV) & (col < PRE_DEV + SUF) & (col - PRE_DEV < slen_ref[0]))
            | (col == PRE_DEV + SUF)
        )
        bias[...] = jnp.where(valid, 0.0, NEG)

        local[0].wait()
        for h in range(HQ):
            q32[h : h + 1, :] = qv[0:1, h * HEAD : (h + 1) * HEAD].astype(F32)
        qsend[0] = q32[0:HALF_HEADS, :].astype(BF16)
        qsend[1] = q32[HALF_HEADS:HQ, :].astype(BF16)

        pad_rows = BLOCK - PRE_DEV - SUF
        first = lax.broadcasted_iota(jnp.int32, (pad_rows, KVH * HEAD), 0) == 0
        local[1].wait()
        kfull[PRE_DEV + SUF : BLOCK, :] = jnp.where(first, knv[0:1, :].astype(F32), 0.0).astype(
            BF16
        )
        local[2].wait()
        vfull[PRE_DEV + SUF : BLOCK, :] = jnp.where(first, vnv[0:1, :].astype(F32), 0.0).astype(
            BF16
        )

    with jax.named_scope("barrier"):
        pl.semaphore_wait(barrier, N - 1)

    with jax.named_scope("qsend"):

        def send_query(i, carry):
            k = i // 2
            half = i % 2
            step = CHIPS // 2 + ((k + 1) // 2) * (1 - 2 * (k % 2))
            target = ((z + step) % CHIPS) * 2 + half
            remote(qsend.at[half], qbuf.at[me], qs_sem, qr_sem.at[my_batch], target).start()
            return carry

        lax.fori_loop(0, N - 2, send_query, 0)
        remote(qsend.at[p], qbuf.at[me], qs_sem, qr_sem.at[my_batch], partner).start()
        pltpu.make_async_copy(qsend.at[c], qbuf.at[me], qr_sem.at[my_batch]).start()

    with jax.named_scope("kvsend"):
        for copy in local[3:7]:
            copy.wait()
        for copy in swaps:
            copy.start()

    with jax.named_scope("resgain"):
        local[7].wait()
        local[8].wait()
        for r in range(D // HEAD):
            res64[r : r + 1, :] = resv[0:1, r * HEAD : (r + 1) * HEAD].astype(F32)
            gain64[r, :] = gainv[r * HEAD : (r + 1) * HEAD].astype(F32)

    with jax.named_scope("kvwait"):
        for copy in swaps[0:3]:
            copy.wait_recv()

    scale = HEAD ** (-0.5)
    row32 = lax.broadcasted_iota(jnp.int32, (RB, BLOCK), 0)
    col32 = lax.broadcasted_iota(jnp.int32, (RB, BLOCK), 1)
    diagonal = col32 % RB == row32

    def attend(b):
        with jax.named_scope("qwait%d" % b):
            wait_bytes(qbuf.at[pl.ds(SB * b, SB)], qr_sem.at[b])
        with jax.named_scope("attn%d" % b):
            queries = nn(
                to_heads[...], qbuf[SB * b : SB * (b + 1)].reshape(SB * HALF_HEADS, HEAD)
            ).astype(BF16)
            shown_own = (col32 < PRE_DEV) | (row32 % SB + SB * b == me)
            shown_par = (col32 < PRE_DEV) | (row32 % SB + SB * b == partner)
            bias_own = jnp.where(shown_own, bias[0:1, :], NEG)
            bias_par = jnp.where(shown_par, bpar[0:1, :], NEG)
            for j in range(HALF_KV):
                qj = queries[RB * j : RB * (j + 1), :]
                own_j = pl.ds(pl.multiple_of(c * HALF_COLS + j * HEAD, HEAD), HEAD)
                s_own = nt(qj, kfull[:, own_j]) * scale + bias_own
                s_par = nt(qj, kpar[:, j * HEAD : (j + 1) * HEAD]) * scale + bias_par
                top = jnp.max(jnp.maximum(s_own, s_par), axis=1, keepdims=True)
                w_own = jnp.exp(s_own - top)
                w_par = jnp.exp(s_par - top)
                total = jnp.sum(w_own + w_par, axis=1, keepdims=True)
                out = nn(w_own.astype(BF16), vfull[:, own_j]) + nn(
                    w_par.astype(BF16), vpar[:, j * HEAD : (j + 1) * HEAD]
                )
                ostage[b, j] = out.astype(BF16)
                sstage[b, j, 0:1, :] = jnp.sum(
                    jnp.where(diagonal, top, 0.0), axis=0, keepdims=True
                )
                sstage[b, j, 1:2, :] = jnp.sum(
                    jnp.where(diagonal, total, 0.0), axis=0, keepdims=True
                )
        with jax.named_scope("osend%d" % b):
            for i in (1, 2, 3, 0):
                j = (z + i) % HALF_CHIPS
                for half in range(2):
                    target = (HALF_CHIPS * c + j) * 2 + half
                    pairs = (
                        (ostage.at[b, j], obuf.at[b, z], os_sem.at[b], or_sem.at[b]),
                        (sstage.at[b, j], sbuf.at[b, z], ss_sem.at[b], sr_sem.at[b]),
                    )
                    if i:
                        for src, dst, ssem, rsem in pairs:
                            remote(src, dst, ssem, rsem, target).start()
                        continue

                    @pl.when(target != me)
                    def _():
                        for src, dst, ssem, rsem in pairs:
                            remote(src, dst, ssem, rsem, target).start()

                    @pl.when(target == me)
                    def _():
                        for src, dst, ssem, rsem in pairs:
                            pltpu.make_async_copy(src, dst, rsem).start()

    def project(b):
        with jax.named_scope("owait%d" % b):
            wait_bytes(obuf.at[b], or_sem.at[b])
            wait_bytes(sbuf.at[b], sr_sem.at[b])
        with jax.named_scope("combine%d" % b):
            stats = sbuf[b]
            group = lax.broadcasted_iota(jnp.int32, (1, BLOCK), 1) // RB
            most = stats[0, 0:1, :]
            for src_z in range(1, CHIPS):
                most = jnp.maximum(most, stats[src_z, 0:1, :])
            summed = jnp.zeros((1, BLOCK), F32)
            factor = jnp.zeros((1, BLOCK), F32)
            for src_z in range(CHIPS):
                f = jnp.exp(stats[src_z, 0:1, :] - most)
                summed = summed + f * stats[src_z, 1:2, :]
                factor = jnp.where(group == src_z, f, factor)
            mix = jnp.where(diagonal, factor / summed, 0.0)
            high = mix.astype(BF16)
            low = (mix - high.astype(F32)).astype(BF16)
            parts = obuf[b].reshape(CHIPS * RB, HEAD)
            attn = nn(high, parts) + nn(low, parts)
            attn = jnp.concatenate([attn[SB * h : SB * (h + 1), :] for h in range(4)], axis=1)
            attn = attn.astype(BF16)
        if b == 0:
            with jax.named_scope("waitw"):
                local[9].wait()
                swaps[3].wait_recv()
        for g in range(GROUPS):
            with jax.named_scope("proj%d%d" % (b, g)):
                at = slice(g * GROUP_COLS, (g + 1) * GROUP_COLS)
                y = nn(attn[:, 0 : 2 * HEAD], wbuf[0, :, at]) + nn(
                    attn[:, 2 * HEAD : 4 * HEAD], wbuf[1, :, at]
                )
                y = jnp.concatenate([y[:, HEAD * i : HEAD * (i + 1)] for i in range(N)], axis=0)
                y = nn(to_samples[...], y.astype(BF16)).astype(BF16)
                ysend[b, g] = y.reshape(SB, N, HEAD)
            with jax.named_scope("ysend%d%d" % (b, g)):

                def send_projection(t, carry):
                    target = SB * b + t

                    @pl.when(target != me)
                    def _():
                        remote(
                            ysend.at[b, g, t], rbuf.at[z, c, g], ys_sem.at[b, g], yr_sem, target
                        ).start()

                    @pl.when(target == me)
                    def _():
                        pltpu.make_async_copy(
                            ysend.at[b, g, t], rbuf.at[z, c, g], yr_sem
                        ).start()

                    return carry

                lax.fori_loop(0, SB, send_projection, 0)

    attend(0)
    attend(1)
    project(0)
    project(1)

    with jax.named_scope("sendwait"):
        wait_bytes(qbuf.at[pl.ds(0, N - 1)], qs_sem)
        for copy in swaps:
            copy.wait_send()

        for b in range(2):
            own_chip = z // HALF_CHIPS == c

            @pl.when(own_chip)
            def _():
                wait_bytes(obuf.at[b, pl.ds(0, CHIPS - 1)], os_sem.at[b])
                wait_bytes(sbuf.at[b, pl.ds(0, CHIPS - 1)], ss_sem.at[b])

            @pl.when(jnp.logical_not(own_chip))
            def _():
                wait_bytes(obuf.at[b], os_sem.at[b])
                wait_bytes(sbuf.at[b], ss_sem.at[b])

    with jax.named_scope("ywait"):
        wait_bytes(rbuf, yr_sem)
    with jax.named_scope("final"):
        stream = res64[...] + jnp.sum(rbuf[...].astype(F32), axis=0).reshape(D // HEAD, HEAD)
        meansq = jnp.sum(stream * stream, keepdims=True) * (1.0 / D)
        normed = stream * lax.rsqrt(meansq + 1e-05) * gain64[...]
        hid_ref[...] = stream.astype(BF16)
        nrm_ref[...] = normed.astype(BF16)
    with jax.named_scope("sendwait2"):
        for b in range(2):
            for g in range(GROUPS):

                @pl.when(my_batch == b)
                def _():
                    wait_bytes(ysend.at[b, g, pl.ds(0, SB - 1)], ys_sem.at[b, g])

                @pl.when(my_batch != b)
                def _():
                    wait_bytes(ysend.at[b, g], ys_sem.at[b, g])


def local(
    query_new,
    key_new,
    value_new,
    prefix_keys,
    prefix_values,
    sample_suffix_keys,
    sample_suffix_values,
    prefix_len,
    suffix_len,
    residual,
    out_weight,
    norm_gain,
):
    hbm = pl.BlockSpec(memory_space=pl.ANY)
    vmem = pl.BlockSpec(memory_space=pltpu.VMEM)
    dma = pltpu.SemaphoreType.DMA
    hidden, normed = pl.pallas_call(
        kernel,
        out_shape=(
            pltpu.VMEM((D // HEAD, HEAD), BF16),
            pltpu.VMEM((D // HEAD, HEAD), BF16),
        ),
        in_specs=[hbm] * 12,
        out_specs=(vmem, vmem),
        scratch_shapes=[
            pltpu.VMEM((1, HQ * HEAD), BF16),
            pltpu.VMEM((1, KVH * HEAD), BF16),
            pltpu.VMEM((1, KVH * HEAD), BF16),
            pltpu.VMEM((1, D), BF16),
            pltpu.VMEM((D,), BF16),
            pltpu.VMEM((BLOCK, KVH * HEAD), BF16),
            pltpu.VMEM((BLOCK, KVH * HEAD), BF16),
            pltpu.VMEM((BLOCK, HALF_COLS), BF16),
            pltpu.VMEM((BLOCK, HALF_COLS), BF16),
            pltpu.VMEM((8, BLOCK), F32),
            pltpu.VMEM((8, BLOCK), F32),
            pltpu.VMEM((HQ, HEAD), F32),
            pltpu.VMEM((2, HALF_HEADS, HEAD), BF16),
            pltpu.VMEM((N, HALF_HEADS, HEAD), BF16),
            pltpu.VMEM((HEAD, HEAD), BF16),
            pltpu.VMEM((HEAD, HEAD), BF16),
            pltpu.VMEM((2, HALF_KV, RB, HEAD), BF16),
            pltpu.VMEM((2, HALF_KV, 2, BLOCK), F32),
            pltpu.VMEM((2, CHIPS, RB, HEAD), BF16),
            pltpu.VMEM((2, CHIPS, 2, BLOCK), F32),
            pltpu.VMEM((2, 2 * HEAD, HALF_D), BF16),
            pltpu.VMEM((2, GROUPS, SB, N, HEAD), BF16),
            pltpu.VMEM((CHIPS, 2, GROUPS, N, HEAD), BF16),
            pltpu.VMEM((D // HEAD, HEAD), F32),
            pltpu.VMEM((D // HEAD, HEAD), F32),
            pltpu.SMEM((1,), jnp.int32),
            pltpu.SMEM((1,), jnp.int32),
            dma((12,)),
            dma,
            dma((2,)),
            dma((4,)),
            dma((4,)),
            dma((2,)),
            dma((2,)),
            dma((2,)),
            dma((2,)),
            dma((2, GROUPS)),
            dma,
        ],
        compiler_params=pltpu.CompilerParams(collective_id=0, has_side_effects=True),
        name="decode_step",
    )(
        query_new,
        key_new,
        value_new,
        prefix_keys,
        prefix_values,
        sample_suffix_keys,
        sample_suffix_values,
        prefix_len,
        suffix_len,
        residual,
        out_weight,
        norm_gain,
    )
    return hidden.reshape(1, D), normed.reshape(1, D)


def solution(mesh):
    placed = (
        P(("dp", "mp"), None),
        P(("dp", "mp"), None),
        P(("dp", "mp"), None),
        P(("dp", "mp"), None),
        P(("dp", "mp"), None),
        P(("dp", "mp"), None, None),
        P(("dp", "mp"), None, None),
        P("dp"),
        P(("dp", "mp")),
        P(("dp", "mp"), None),
        P("mp", None),
        P(),
    )
    return jax.shard_map(
        local,
        mesh=mesh,
        in_specs=placed,
        out_specs=(P(("dp", "mp"), None), P(("dp", "mp"), None)),
        check_vma=False,
    )
```

```python
import functools

import jax
import jax.numpy as jnp
from jax import lax
from jax.experimental import pallas as pl
from jax.experimental.pallas import tpu as pltpu
from jax.sharding import PartitionSpec as P

HEAD = 128
KVH = 8
HQ = 32
D = 8192
CHIPS = 8
N = 16
HALF_HEADS = 16
HALF_KV = 4
PRE_DEV = 128
SUF = 64
BLOCK = 256
HALF_COLS = HALF_KV * HEAD
HALF_D = D // 2
GROUPS = 2
GROUP_COLS = HALF_D // GROUPS
NEG = -1e30
F32 = jnp.float32
BF16 = jnp.bfloat16
HALF_CHIPS = CHIPS // 2
BATCHES = ((0, 4), (4, 4), (8, 8))
NB = len(BATCHES)
SB = 8
RB = 4 * SB


def nt(a, b):
    return lax.dot_general(a, b, (((1,), (1,)), ((), ())), preferred_element_type=F32)


def nn(a, b):
    return lax.dot_general(a, b, (((1,), (0,)), ((), ())), preferred_element_type=F32)


def kernel(
    q_hbm,
    kn_hbm,
    vn_hbm,
    pk_hbm,
    pv_hbm,
    sk_hbm,
    sv_hbm,
    plen_hbm,
    slen_hbm,
    res_hbm,
    w_hbm,
    gain_hbm,
    hid_ref,
    nrm_ref,
    qv,
    knv,
    vnv,
    resv,
    gainv,
    kfull,
    vfull,
    kpar,
    vpar,
    bias,
    bpar,
    q32,
    qsend,
    qbuf,
    to_heads,
    to_samples,
    ostage,
    sstage,
    obuf,
    sbuf,
    wbuf,
    ysend,
    rbuf,
    res64,
    gain64,
    plen_ref,
    slen_ref,
    loc_sem,
    qs_sem,
    qr_sem,
    xs_sem,
    xr_sem,
    os_sem,
    or_sem,
    ss_sem,
    sr_sem,
    ys_sem,
    yr_sem,
):
    me = lax.axis_index("mp")
    z = me // 2
    c = me % 2
    p = 1 - c
    partner = z * 2 + p
    my_batch = z // 2 - z // 6

    def at_mp(index):
        return {"mp": index}

    def remote(src, dst, ssem, rsem, index):
        return pltpu.make_async_remote_copy(
            src_ref=src,
            dst_ref=dst,
            send_sem=ssem,
            recv_sem=rsem,
            device_id=at_mp(index),
            device_id_type=pl.DeviceIdType.MESH,
        )

    def wait_bytes(ref, sem):
        pltpu.make_async_copy(ref, ref, sem).wait()

    own_cols = pl.ds(pl.multiple_of(c * HALF_COLS, HALF_COLS), HALF_COLS)
    par_cols = pl.ds(pl.multiple_of(p * HALF_COLS, HALF_COLS), HALF_COLS)
    own_d = pl.ds(pl.multiple_of(c * HALF_D, HALF_D), HALF_D)
    par_d = pl.ds(pl.multiple_of(p * HALF_D, HALF_D), HALF_D)
    swaps = [
        remote(kfull.at[:, par_cols], kpar, xs_sem.at[0], xr_sem.at[0], partner),
        remote(vfull.at[:, par_cols], vpar, xs_sem.at[1], xr_sem.at[1], partner),
        remote(bias, bpar, xs_sem.at[2], xr_sem.at[2], partner),
        remote(w_hbm.at[:, par_d], wbuf.at[c], xs_sem.at[3], xr_sem.at[3], partner),
    ]
    local = [
        pltpu.make_async_copy(q_hbm, qv, loc_sem.at[0]),
        pltpu.make_async_copy(kn_hbm, knv, loc_sem.at[1]),
        pltpu.make_async_copy(vn_hbm, vnv, loc_sem.at[2]),
        pltpu.make_async_copy(pk_hbm, kfull.at[pl.ds(0, PRE_DEV)], loc_sem.at[3]),
        pltpu.make_async_copy(pv_hbm, vfull.at[pl.ds(0, PRE_DEV)], loc_sem.at[4]),
        pltpu.make_async_copy(sk_hbm.at[0], kfull.at[pl.ds(PRE_DEV, SUF)], loc_sem.at[5]),
        pltpu.make_async_copy(sv_hbm.at[0], vfull.at[pl.ds(PRE_DEV, SUF)], loc_sem.at[6]),
        pltpu.make_async_copy(res_hbm, resv, loc_sem.at[7]),
        pltpu.make_async_copy(gain_hbm, gainv, loc_sem.at[8]),
        pltpu.make_async_copy(w_hbm.at[:, own_d], wbuf.at[c], loc_sem.at[9]),
        pltpu.make_async_copy(plen_hbm, plen_ref, loc_sem.at[10]),
        pltpu.make_async_copy(slen_hbm, slen_ref, loc_sem.at[11]),
    ]

    with jax.named_scope("prep"):
        barrier = pltpu.get_barrier_semaphore()

        for step in (4, 3, 5, 2, 6, 1, 7):
            for half in (0, 1):
                pl.semaphore_signal(
                    barrier,
                    inc=1,
                    device_id=at_mp(((z + step) % CHIPS) * 2 + half),
                    device_id_type=pl.DeviceIdType.MESH,
                )
        pl.semaphore_signal(
            barrier, inc=1, device_id=at_mp(partner), device_id_type=pl.DeviceIdType.MESH
        )
        for copy in local:
            copy.start()

        rows = lax.broadcasted_iota(jnp.int32, (HEAD, HEAD), 0)
        cols = lax.broadcasted_iota(jnp.int32, (HEAD, HEAD), 1)
        for i, ns in enumerate((4, 8)):
            to_heads[i] = jnp.where(cols == (rows % ns) * N + rows // ns, 1.0, 0.0).astype(BF16)
        to_samples[...] = jnp.where(cols == (rows % N) * SB + rows // N, 1.0, 0.0).astype(BF16)
        local[10].wait()
        local[11].wait()
        col = lax.broadcasted_iota(jnp.int32, (8, BLOCK), 1)
        valid = (
            ((col < PRE_DEV) & (col + me * PRE_DEV < plen_ref[0]))
            | ((col >= PRE_DEV) & (col < PRE_DEV + SUF) & (col - PRE_DEV < slen_ref[0]))
            | (col == PRE_DEV + SUF)
        )
        bias[...] = jnp.where(valid, 0.0, NEG)

        local[0].wait()
        for h in range(HQ):
            q32[h : h + 1, :] = qv[0:1, h * HEAD : (h + 1) * HEAD].astype(F32)
        qsend[0] = q32[0:HALF_HEADS, :].astype(BF16)
        qsend[1] = q32[HALF_HEADS:HQ, :].astype(BF16)

        pad_rows = BLOCK - PRE_DEV - SUF
        first = lax.broadcasted_iota(jnp.int32, (pad_rows, KVH * HEAD), 0) == 0
        local[1].wait()
        kfull[PRE_DEV + SUF : BLOCK, :] = jnp.where(first, knv[0:1, :].astype(F32), 0.0).astype(
            BF16
        )
        local[2].wait()
        vfull[PRE_DEV + SUF : BLOCK, :] = jnp.where(first, vnv[0:1, :].astype(F32), 0.0).astype(
            BF16
        )

    with jax.named_scope("barrier"):
        pl.semaphore_wait(barrier, N - 1)

    with jax.named_scope("qsend"):

        def send_query(i, carry):
            k = i // 2
            half = i % 2
            step = CHIPS // 2 + ((k + 1) // 2) * (1 - 2 * (k % 2))
            target = ((z + step) % CHIPS) * 2 + half
            remote(qsend.at[half], qbuf.at[me], qs_sem, qr_sem.at[my_batch], target).start()
            return carry

        lax.fori_loop(0, N - 2, send_query, 0)
        remote(qsend.at[p], qbuf.at[me], qs_sem, qr_sem.at[my_batch], partner).start()
        pltpu.make_async_copy(qsend.at[c], qbuf.at[me], qr_sem.at[my_batch]).start()

    with jax.named_scope("kvsend"):
        for copy in local[3:7]:
            copy.wait()
        for copy in swaps:
            copy.start()

    with jax.named_scope("resgain"):
        local[7].wait()
        local[8].wait()
        for r in range(D // HEAD):
            res64[r : r + 1, :] = resv[0:1, r * HEAD : (r + 1) * HEAD].astype(F32)
            gain64[r, :] = gainv[r * HEAD : (r + 1) * HEAD].astype(F32)

    with jax.named_scope("kvwait"):
        for copy in swaps[0:3]:
            copy.wait_recv()

    scale = HEAD ** (-0.5)

    def diagonal(ns):
        rows = lax.broadcasted_iota(jnp.int32, (4 * ns, 32 * ns), 0)
        cols = lax.broadcasted_iota(jnp.int32, (4 * ns, 32 * ns), 1)
        return cols % (4 * ns) == rows

    def attend(b):
        start, ns = BATCHES[b]
        rb = 4 * ns
        with jax.named_scope("qwait%d" % b):
            wait_bytes(qbuf.at[pl.ds(start, ns)], qr_sem.at[b])
        with jax.named_scope("attn%d" % b):
            size = ns * HALF_HEADS
            queries = nn(
                to_heads[ns // 8, 0:size, 0:size],
                qbuf[start : start + ns].reshape(size, HEAD),
            ).astype(BF16)
            sample = lax.broadcasted_iota(jnp.int32, (rb, BLOCK), 0) % ns + start
            shared = lax.broadcasted_iota(jnp.int32, (rb, BLOCK), 1) < PRE_DEV
            bias_own = jnp.where(shared | (sample == me), bias[0:1, :], NEG)
            bias_par = jnp.where(shared | (sample == partner), bpar[0:1, :], NEG)
            scores = []
            for j in range(HALF_KV):
                qj = queries[rb * j : rb * (j + 1), :]
                at_own = pl.ds(pl.multiple_of(c * HALF_COLS + j * HEAD, HEAD), HEAD)
                scores.append(
                    (
                        nt(qj, kfull[:, at_own]) * scale + bias_own,
                        nt(qj, kpar[:, j * HEAD : (j + 1) * HEAD]) * scale + bias_par,
                    )
                )
            tops = [jnp.max(jnp.maximum(x, y), axis=1, keepdims=True) for x, y in scores]
            weights = [(jnp.exp(x - t), jnp.exp(y - t)) for (x, y), t in zip(scores, tops)]
            totals = [jnp.sum(x + y, axis=1, keepdims=True) for x, y in weights]
            for j in range(HALF_KV):
                at_own = pl.ds(pl.multiple_of(c * HALF_COLS + j * HEAD, HEAD), HEAD)
                w_own, w_par = weights[j]
                out = nn(w_own.astype(BF16), vfull[:, at_own]) + nn(
                    w_par.astype(BF16), vpar[:, j * HEAD : (j + 1) * HEAD]
                )
                ostage[b, j, 0:rb, :] = out.astype(BF16)
            for j in range(HALF_KV):
                for i, stat in enumerate((tops[j], totals[j])):
                    sstage[b, j, i : i + 1, 0 : 8 * rb] = jnp.sum(
                        jnp.where(diagonal(ns), stat, 0.0), axis=0, keepdims=True
                    )
        with jax.named_scope("osend%d" % b):
            for i in (1, 2, 3, 0):
                j = (z + i) % HALF_CHIPS
                for half in range(2):
                    target = (HALF_CHIPS * c + j) * 2 + half
                    pairs = (
                        (
                            ostage.at[b, j, pl.ds(0, rb)],
                            obuf.at[b, z, pl.ds(0, rb)],
                            os_sem.at[b],
                            or_sem.at[b],
                        ),
                        (
                            sstage.at[b, j, :, pl.ds(0, 8 * rb)],
                            sbuf.at[b, z, :, pl.ds(0, 8 * rb)],
                            ss_sem.at[b],
                            sr_sem.at[b],
                        ),
                    )
                    if i:
                        for src, dst, ssem, rsem in pairs:
                            remote(src, dst, ssem, rsem, target).start()
                        continue

                    @pl.when(target != me)
                    def _():
                        for src, dst, ssem, rsem in pairs:
                            remote(src, dst, ssem, rsem, target).start()

                    @pl.when(target == me)
                    def _():
                        for src, dst, ssem, rsem in pairs:
                            pltpu.make_async_copy(src, dst, rsem).start()

    def project(b):
        start, ns = BATCHES[b]
        rb = 4 * ns
        with jax.named_scope("owait%d" % b):
            wait_bytes(obuf.at[b, :, pl.ds(0, rb)], or_sem.at[b])
            wait_bytes(sbuf.at[b, :, :, pl.ds(0, 8 * rb)], sr_sem.at[b])
        with jax.named_scope("combine%d" % b):
            stats = sbuf[b, :, :, 0 : 8 * rb]
            group = lax.broadcasted_iota(jnp.int32, (1, 8 * rb), 1) // rb
            most = stats[0, 0:1, :]
            for src_z in range(1, CHIPS):
                most = jnp.maximum(most, stats[src_z, 0:1, :])
            summed = jnp.zeros((1, 8 * rb), F32)
            factor = jnp.zeros((1, 8 * rb), F32)
            for src_z in range(CHIPS):
                f = jnp.exp(stats[src_z, 0:1, :] - most)
                summed = summed + f * stats[src_z, 1:2, :]
                factor = jnp.where(group == src_z, f, factor)
            mix = jnp.where(diagonal(ns), factor / summed, 0.0)
            high = mix.astype(BF16)
            low = (mix - high.astype(F32)).astype(BF16)
            parts = obuf[b, :, 0:rb, :].reshape(CHIPS * rb, HEAD)
            attn = nn(high, parts) + nn(low, parts)
            attn = jnp.concatenate([attn[ns * h : ns * (h + 1), :] for h in range(4)], axis=1)
            if ns < SB:
                attn = jnp.concatenate([attn, jnp.zeros((SB - ns, 4 * HEAD), F32)], axis=0)
            attn = attn.astype(BF16)
        if b == 0:
            with jax.named_scope("waitw"):
                local[9].wait()
                swaps[3].wait_recv()
        for g in range(GROUPS):
            with jax.named_scope("proj%d%d" % (b, g)):
                at = slice(g * GROUP_COLS, (g + 1) * GROUP_COLS)
                y = nn(attn[:, 0 : 2 * HEAD], wbuf[0, :, at]) + nn(
                    attn[:, 2 * HEAD : 4 * HEAD], wbuf[1, :, at]
                )
                y = jnp.concatenate([y[:, HEAD * i : HEAD * (i + 1)] for i in range(N)], axis=0)
                y = nn(to_samples[...], y.astype(BF16)).astype(BF16)
                ysend[b, g] = y.reshape(SB, N, HEAD)
            with jax.named_scope("ysend%d%d" % (b, g)):

                def send_projection(t, carry):
                    target = start + t

                    @pl.when(target != me)
                    def _():
                        remote(
                            ysend.at[b, g, t], rbuf.at[z, c, g], ys_sem.at[b, g], yr_sem, target
                        ).start()

                    @pl.when(target == me)
                    def _():
                        pltpu.make_async_copy(
                            ysend.at[b, g, t], rbuf.at[z, c, g], yr_sem
                        ).start()

                    return carry

                lax.fori_loop(0, ns, send_projection, 0)

    for b in range(NB):
        attend(b)
    for b in range(NB):
        project(b)

    with jax.named_scope("sendwait"):
        wait_bytes(qbuf.at[pl.ds(0, N - 1)], qs_sem)
        for copy in swaps:
            copy.wait_send()

        for b, (start, ns) in enumerate(BATCHES):
            own_chip = z // HALF_CHIPS == c
            for here, count in ((own_chip, CHIPS - 1), (jnp.logical_not(own_chip), CHIPS)):

                @pl.when(here)
                def _():
                    wait_bytes(obuf.at[b, pl.ds(0, count), pl.ds(0, 4 * ns)], os_sem.at[b])
                    wait_bytes(sbuf.at[b, pl.ds(0, count), :, pl.ds(0, 32 * ns)], ss_sem.at[b])

    with jax.named_scope("ywait"):
        wait_bytes(rbuf, yr_sem)
    with jax.named_scope("final"):
        stream = res64[...] + jnp.sum(rbuf[...].astype(F32), axis=0).reshape(D // HEAD, HEAD)
        meansq = jnp.sum(stream * stream, keepdims=True) * (1.0 / D)
        normed = stream * lax.rsqrt(meansq + 1e-05) * gain64[...]
        hid_ref[...] = stream.astype(BF16)
        nrm_ref[...] = normed.astype(BF16)
    with jax.named_scope("sendwait2"):
        for b, (start, ns) in enumerate(BATCHES):
            for g in range(GROUPS):

                @pl.when(my_batch == b)
                def _():
                    wait_bytes(ysend.at[b, g, pl.ds(0, ns - 1)], ys_sem.at[b, g])

                @pl.when(my_batch != b)
                def _():
                    wait_bytes(ysend.at[b, g, pl.ds(0, ns)], ys_sem.at[b, g])


def local(
    query_new,
    key_new,
    value_new,
    prefix_keys,
    prefix_values,
    sample_suffix_keys,
    sample_suffix_values,
    prefix_len,
    suffix_len,
    residual,
    out_weight,
    norm_gain,
):
    hbm = pl.BlockSpec(memory_space=pl.ANY)
    vmem = pl.BlockSpec(memory_space=pltpu.VMEM)
    dma = pltpu.SemaphoreType.DMA
    hidden, normed = pl.pallas_call(
        kernel,
        out_shape=(
            pltpu.VMEM((D // HEAD, HEAD), BF16),
            pltpu.VMEM((D // HEAD, HEAD), BF16),
        ),
        in_specs=[hbm] * 12,
        out_specs=(vmem, vmem),
        scratch_shapes=[
            pltpu.VMEM((1, HQ * HEAD), BF16),
            pltpu.VMEM((1, KVH * HEAD), BF16),
            pltpu.VMEM((1, KVH * HEAD), BF16),
            pltpu.VMEM((1, D), BF16),
            pltpu.VMEM((D,), BF16),
            pltpu.VMEM((BLOCK, KVH * HEAD), BF16),
            pltpu.VMEM((BLOCK, KVH * HEAD), BF16),
            pltpu.VMEM((BLOCK, HALF_COLS), BF16),
            pltpu.VMEM((BLOCK, HALF_COLS), BF16),
            pltpu.VMEM((8, BLOCK), F32),
            pltpu.VMEM((8, BLOCK), F32),
            pltpu.VMEM((HQ, HEAD), F32),
            pltpu.VMEM((2, HALF_HEADS, HEAD), BF16),
            pltpu.VMEM((N, HALF_HEADS, HEAD), BF16),
            pltpu.VMEM((2, HEAD, HEAD), BF16),
            pltpu.VMEM((HEAD, HEAD), BF16),
            pltpu.VMEM((NB, HALF_KV, RB, HEAD), BF16),
            pltpu.VMEM((NB, HALF_KV, 2, BLOCK), F32),
            pltpu.VMEM((NB, CHIPS, RB, HEAD), BF16),
            pltpu.VMEM((NB, CHIPS, 2, BLOCK), F32),
            pltpu.VMEM((2, 2 * HEAD, HALF_D), BF16),
            pltpu.VMEM((NB, GROUPS, SB, N, HEAD), BF16),
            pltpu.VMEM((CHIPS, 2, GROUPS, N, HEAD), BF16),
            pltpu.VMEM((D // HEAD, HEAD), F32),
            pltpu.VMEM((D // HEAD, HEAD), F32),
            pltpu.SMEM((1,), jnp.int32),
            pltpu.SMEM((1,), jnp.int32),
            dma((12,)),
            dma,
            dma((NB,)),
            dma((4,)),
            dma((4,)),
            dma((NB,)),
            dma((NB,)),
            dma((NB,)),
            dma((NB,)),
            dma((NB, GROUPS)),
            dma,
        ],
        compiler_params=pltpu.CompilerParams(collective_id=0, has_side_effects=True),
        name="decode_step",
    )(
        query_new,
        key_new,
        value_new,
        prefix_keys,
        prefix_values,
        sample_suffix_keys,
        sample_suffix_values,
        prefix_len,
        suffix_len,
        residual,
        out_weight,
        norm_gain,
    )
    return hidden.reshape(1, D), normed.reshape(1, D)


def solution(mesh):
    placed = (
        P(("dp", "mp"), None),
        P(("dp", "mp"), None),
        P(("dp", "mp"), None),
        P(("dp", "mp"), None),
        P(("dp", "mp"), None),
        P(("dp", "mp"), None, None),
        P(("dp", "mp"), None, None),
        P("dp"),
        P(("dp", "mp")),
        P(("dp", "mp"), None),
        P("mp", None),
        P(),
    )
    return jax.shard_map(
        local,
        mesh=mesh,
        in_specs=placed,
        out_specs=(P(("dp", "mp"), None), P(("dp", "mp"), None)),
        check_vma=False,
    )
```

```python
import functools

import jax
import jax.numpy as jnp
from jax import lax
from jax.experimental import pallas as pl
from jax.experimental.pallas import tpu as pltpu
from jax.sharding import PartitionSpec as P

HEAD = 128
KVH = 8
HQ = 32
D = 8192
CHIPS = 8
N = 16
HALF_HEADS = 16
HALF_KV = 4
PRE_DEV = 128
SUF = 64
BLOCK = 256
HALF_COLS = HALF_KV * HEAD
HALF_D = D // 2
NEG = -1e30
F32 = jnp.float32
BF16 = jnp.bfloat16
HALF_CHIPS = CHIPS // 2
BATCHES = ((0, 4), (4, 4), (8, 8))
NB = len(BATCHES)
SB = 8
RB = 4 * SB


def nt(a, b):
    return lax.dot_general(a, b, (((1,), (1,)), ((), ())), preferred_element_type=F32)


def nn(a, b):
    return lax.dot_general(a, b, (((1,), (0,)), ((), ())), preferred_element_type=F32)


def kernel(
    q_hbm,
    kn_hbm,
    vn_hbm,
    pk_hbm,
    pv_hbm,
    sk_hbm,
    sv_hbm,
    plen_hbm,
    slen_hbm,
    res_hbm,
    w_hbm,
    gain_hbm,
    hid_ref,
    nrm_ref,
    qv,
    knv,
    vnv,
    resv,
    gainv,
    kfull,
    vfull,
    kpar,
    vpar,
    bias,
    bpar,
    q32,
    qsend,
    qbuf,
    to_heads,
    to_samples,
    ostage,
    sstage,
    obuf,
    sbuf,
    wbuf,
    ysend,
    rbuf,
    res64,
    gain64,
    plen_ref,
    slen_ref,
    bytes_ref,
    loc_sem,
    send_sem,
    qr_sem,
    xr_sem,
    or_sem,
    yr_sem,
):
    me = lax.axis_index("mp")
    z = me // 2
    c = me % 2
    p = 1 - c
    partner = z * 2 + p
    own_half = p
    par_half = c
    my_batch = z // 2 - z // 6

    def at_mp(index):
        return {"mp": index}

    def remote(src, dst, rsem, index):
        return pltpu.make_async_remote_copy(
            src_ref=src,
            dst_ref=dst,
            send_sem=send_sem,
            recv_sem=rsem,
            device_id=at_mp(index),
            device_id_type=pl.DeviceIdType.MESH,
        )

    def wait_total(size, sem):
        wait_bytes(bytes_ref.at[pl.ds(0, size // (4 * HEAD))], sem)

    def wait_bytes(ref, sem):
        pltpu.make_async_copy(ref, ref, sem).wait()

    par_cols = pl.ds(pl.multiple_of(par_half * HALF_COLS, HALF_COLS), HALF_COLS)
    own_d = pl.ds(pl.multiple_of(c * HALF_D, HALF_D), HALF_D)
    par_d = pl.ds(pl.multiple_of(p * HALF_D, HALF_D), HALF_D)
    swaps = [
        remote(kfull.at[:, par_cols], kpar, xr_sem.at[0], partner),
        remote(vfull.at[:, par_cols], vpar, xr_sem.at[0], partner),
        remote(bias, bpar, xr_sem.at[0], partner),
        remote(w_hbm.at[:, par_d], wbuf.at[c], xr_sem.at[1], partner),
    ]
    local = [
        pltpu.make_async_copy(q_hbm, qv, loc_sem.at[0]),
        pltpu.make_async_copy(kn_hbm, knv, loc_sem.at[1]),
        pltpu.make_async_copy(vn_hbm, vnv, loc_sem.at[8]),
        pltpu.make_async_copy(pk_hbm, kfull.at[pl.ds(0, PRE_DEV)], loc_sem.at[2]),
        pltpu.make_async_copy(pv_hbm, vfull.at[pl.ds(0, PRE_DEV)], loc_sem.at[2]),
        pltpu.make_async_copy(sk_hbm.at[0], kfull.at[pl.ds(PRE_DEV, SUF)], loc_sem.at[2]),
        pltpu.make_async_copy(sv_hbm.at[0], vfull.at[pl.ds(PRE_DEV, SUF)], loc_sem.at[2]),
        pltpu.make_async_copy(res_hbm, resv, loc_sem.at[3]),
        pltpu.make_async_copy(gain_hbm, gainv, loc_sem.at[4]),
        pltpu.make_async_copy(w_hbm.at[:, own_d], wbuf.at[c], loc_sem.at[5]),
        pltpu.make_async_copy(plen_hbm, plen_ref, loc_sem.at[6]),
        pltpu.make_async_copy(slen_hbm, slen_ref, loc_sem.at[7]),
    ]

    with jax.named_scope("prep"):
        barrier = pltpu.get_barrier_semaphore()

        for step in (4, 3, 5, 2, 6, 1, 7):
            for half in (0, 1):
                pl.semaphore_signal(
                    barrier,
                    inc=1,
                    device_id=at_mp(((z + step) % CHIPS) * 2 + half),
                    device_id_type=pl.DeviceIdType.MESH,
                )
        pl.semaphore_signal(
            barrier, inc=1, device_id=at_mp(partner), device_id_type=pl.DeviceIdType.MESH
        )
        for copy in local:
            copy.start()

        rows = lax.broadcasted_iota(jnp.int32, (HEAD, HEAD), 0)
        cols = lax.broadcasted_iota(jnp.int32, (HEAD, HEAD), 1)
        for i, ns in enumerate((4, 8)):
            to_heads[i] = jnp.where(cols == (rows % ns) * N + rows // ns, 1.0, 0.0).astype(BF16)
        to_samples[...] = jnp.where(cols == (rows % N) * SB + rows // N, 1.0, 0.0).astype(BF16)
        local[10].wait()
        local[11].wait()
        col = lax.broadcasted_iota(jnp.int32, (8, BLOCK), 1)
        valid = (
            ((col < PRE_DEV) & (col + me * PRE_DEV < plen_ref[0]))
            | ((col >= PRE_DEV) & (col < PRE_DEV + SUF) & (col - PRE_DEV < slen_ref[0]))
            | (col == PRE_DEV + SUF)
        )
        bias[...] = jnp.where(valid, 0.0, NEG)

        local[0].wait()
        for h in range(HQ):
            q32[h : h + 1, :] = qv[0:1, h * HEAD : (h + 1) * HEAD].astype(F32)
        qsend[0] = q32[0:HALF_HEADS, :].astype(BF16)
        qsend[1] = q32[HALF_HEADS:HQ, :].astype(BF16)

        pad_rows = BLOCK - PRE_DEV - SUF
        first = lax.broadcasted_iota(jnp.int32, (pad_rows, KVH * HEAD), 0) == 0
        local[1].wait()
        kfull[PRE_DEV + SUF : BLOCK, :] = jnp.where(first, knv[0:1, :].astype(F32), 0.0).astype(
            BF16
        )
        local[2].wait()
        vfull[PRE_DEV + SUF : BLOCK, :] = jnp.where(first, vnv[0:1, :].astype(F32), 0.0).astype(
            BF16
        )

    with jax.named_scope("barrier"):
        pl.semaphore_wait(barrier, N - 1)

    with jax.named_scope("qsend"):

        def send_query(i, carry):
            k = i // 2
            half = i % 2
            step = CHIPS // 2 + ((k + 1) // 2) * (1 - 2 * (k % 2))
            target = ((z + step) % CHIPS) * 2 + 1 - half
            remote(qsend.at[half], qbuf.at[me], qr_sem.at[my_batch], target).start()
            return carry

        lax.fori_loop(0, N - 2, send_query, 0)
        remote(qsend.at[par_half], qbuf.at[me], qr_sem.at[my_batch], partner).start()
        pltpu.make_async_copy(qsend.at[own_half], qbuf.at[me], qr_sem.at[my_batch]).start()

    with jax.named_scope("kvsend"):
        wait_total(2 * 2 * (PRE_DEV + SUF) * KVH * HEAD, loc_sem.at[2])
        for copy in swaps:
            copy.start()

    with jax.named_scope("resgain"):
        local[7].wait()
        local[8].wait()
        for r in range(D // HEAD):
            res64[r : r + 1, :] = resv[0:1, r * HEAD : (r + 1) * HEAD].astype(F32)
            gain64[r, :] = gainv[r * HEAD : (r + 1) * HEAD].astype(F32)

    with jax.named_scope("kvwait"):
        wait_total(2 * 2 * BLOCK * HALF_COLS + 4 * 8 * BLOCK, xr_sem.at[0])

    scale = HEAD ** (-0.5)

    def diagonal(ns):
        rows = lax.broadcasted_iota(jnp.int32, (4 * ns, 32 * ns), 0)
        cols = lax.broadcasted_iota(jnp.int32, (4 * ns, 32 * ns), 1)
        return cols % (4 * ns) == rows

    def sums_bytes(ns):
        return 2 * 4 * ns * HEAD + 4 * 2 * 32 * ns

    def attend(b):
        start, ns = BATCHES[b]
        rb = 4 * ns
        with jax.named_scope("qwait%d" % b):
            wait_bytes(qbuf.at[pl.ds(start, ns)], qr_sem.at[b])
        with jax.named_scope("attn%d" % b):
            size = ns * HALF_HEADS
            queries = nn(
                to_heads[ns // 8, 0:size, 0:size],
                qbuf[start : start + ns].reshape(size, HEAD),
            ).astype(BF16)
            sample = lax.broadcasted_iota(jnp.int32, (rb, BLOCK), 0) % ns + start
            shared = lax.broadcasted_iota(jnp.int32, (rb, BLOCK), 1) < PRE_DEV
            bias_own = jnp.where(shared | (sample == me), bias[0:1, :], NEG)
            bias_par = jnp.where(shared | (sample == partner), bpar[0:1, :], NEG)
            scores = []
            for j in range(HALF_KV):
                qj = queries[rb * j : rb * (j + 1), :]
                at_own = pl.ds(pl.multiple_of(own_half * HALF_COLS + j * HEAD, HEAD), HEAD)
                scores.append(
                    (
                        nt(qj, kfull[:, at_own]) * scale + bias_own,
                        nt(qj, kpar[:, j * HEAD : (j + 1) * HEAD]) * scale + bias_par,
                    )
                )
            tops = [jnp.max(jnp.maximum(x, y), axis=1, keepdims=True) for x, y in scores]
            weights = [(jnp.exp(x - t), jnp.exp(y - t)) for (x, y), t in zip(scores, tops)]
            totals = [jnp.sum(x + y, axis=1, keepdims=True) for x, y in weights]
            for j in range(HALF_KV):
                at_own = pl.ds(pl.multiple_of(own_half * HALF_COLS + j * HEAD, HEAD), HEAD)
                w_own, w_par = weights[j]
                out = nn(w_own.astype(BF16), vfull[:, at_own]) + nn(
                    w_par.astype(BF16), vpar[:, j * HEAD : (j + 1) * HEAD]
                )
                ostage[b, j, 0:rb, :] = out.astype(BF16)
            for j in range(HALF_KV):
                for i, stat in enumerate((tops[j], totals[j])):
                    sstage[b, j, i : i + 1, 0 : 8 * rb] = jnp.sum(
                        jnp.where(diagonal(ns), stat, 0.0), axis=0, keepdims=True
                    )
        with jax.named_scope("osend%d" % b):
            for i in (1, 2, 3, 0):
                j = (z + i) % HALF_CHIPS
                for half in range(2):
                    target = (HALF_CHIPS * own_half + j) * 2 + half
                    pairs = (
                        (ostage.at[b, j, pl.ds(0, rb)], obuf.at[b, z, pl.ds(0, rb)]),
                        (
                            sstage.at[b, j, :, pl.ds(0, 8 * rb)],
                            sbuf.at[b, z, :, pl.ds(0, 8 * rb)],
                        ),
                    )
                    if i:
                        for src, dst in pairs:
                            remote(src, dst, or_sem.at[b], target).start()
                        continue

                    @pl.when(target != me)
                    def _():
                        for src, dst in pairs:
                            remote(src, dst, or_sem.at[b], target).start()

                    @pl.when(target == me)
                    def _():
                        for src, dst in pairs:
                            pltpu.make_async_copy(src, dst, or_sem.at[b]).start()

    def project(b):
        start, ns = BATCHES[b]
        rb = 4 * ns
        with jax.named_scope("owait%d" % b):
            wait_total(CHIPS * sums_bytes(ns), or_sem.at[b])
        with jax.named_scope("combine%d" % b):
            stats = sbuf[b, :, :, 0 : 8 * rb]
            group = lax.broadcasted_iota(jnp.int32, (1, 8 * rb), 1) // rb
            most = stats[0, 0:1, :]
            for src_z in range(1, CHIPS):
                most = jnp.maximum(most, stats[src_z, 0:1, :])
            summed = jnp.zeros((1, 8 * rb), F32)
            factor = jnp.zeros((1, 8 * rb), F32)
            for src_z in range(CHIPS):
                f = jnp.exp(stats[src_z, 0:1, :] - most)
                summed = summed + f * stats[src_z, 1:2, :]
                factor = jnp.where(group == src_z, f, factor)
            mix = jnp.where(diagonal(ns), factor / summed, 0.0)
            high = mix.astype(BF16)
            low = (mix - high.astype(F32)).astype(BF16)
            parts = obuf[b, :, 0:rb, :].reshape(CHIPS * rb, HEAD)
            attn = nn(high, parts) + nn(low, parts)
            attn = jnp.concatenate([attn[ns * h : ns * (h + 1), :] for h in range(4)], axis=1)
            if ns < SB:
                attn = jnp.concatenate([attn, jnp.zeros((SB - ns, 4 * HEAD), F32)], axis=0)
            attn = attn.astype(BF16)
        if b == 0:
            with jax.named_scope("waitw"):
                local[9].wait()
                swaps[3].wait_recv()
        with jax.named_scope("proj%d" % b):
            y = nn(attn[:, 0 : 2 * HEAD], wbuf[0]) + nn(attn[:, 2 * HEAD : 4 * HEAD], wbuf[1])
            for g in range(2):
                part = [y[:, HEAD * i : HEAD * (i + 1)] for i in range(N * g, N * (g + 1))]
                part = jnp.concatenate(part, axis=0).astype(BF16)
                part = nn(to_samples[...], part).astype(BF16)
                ysend[b, :, N * g : N * (g + 1), :] = part.reshape(SB, N, HEAD)
        with jax.named_scope("ysend%d" % b):

            def send_projection(t, carry):
                target = start + t

                @pl.when(target != me)
                def _():
                    remote(ysend.at[b, t], rbuf.at[z, c], yr_sem, target).start()

                @pl.when(target == me)
                def _():
                    pltpu.make_async_copy(ysend.at[b, t], rbuf.at[z, c], yr_sem).start()

                return carry

            lax.fori_loop(0, ns, send_projection, 0)

    for b in (0, 2, 1):
        attend(b)
    for b in (0, 2, 1):
        project(b)

    with jax.named_scope("ywait"):
        wait_bytes(rbuf, yr_sem)
    with jax.named_scope("final"):
        stream = res64[...] + jnp.sum(rbuf[...].astype(F32), axis=0).reshape(D // HEAD, HEAD)
        meansq = jnp.sum(stream * stream, keepdims=True) * (1.0 / D)
        normed = stream * lax.rsqrt(meansq + 1e-05) * gain64[...]
        hid_ref[...] = stream.astype(BF16)
        nrm_ref[...] = normed.astype(BF16)
    with jax.named_scope("sendwait"):
        sent = (N - 1) * 2 * HALF_HEADS * HEAD
        sent += 2 * 2 * BLOCK * HALF_COLS + 4 * 8 * BLOCK + 2 * 2 * HEAD * HALF_D
        sent += sum(2 * HALF_CHIPS * sums_bytes(ns) for _, ns in BATCHES)
        sent += (N - 1) * 2 * HALF_D
        own_chip = z // HALF_CHIPS == own_half

        @pl.when(own_chip)
        def _():
            wait_total(sent - sum(sums_bytes(ns) for _, ns in BATCHES), send_sem)

        @pl.when(jnp.logical_not(own_chip))
        def _():
            wait_total(sent, send_sem)


def local(
    query_new,
    key_new,
    value_new,
    prefix_keys,
    prefix_values,
    sample_suffix_keys,
    sample_suffix_values,
    prefix_len,
    suffix_len,
    residual,
    out_weight,
    norm_gain,
):
    hbm = pl.BlockSpec(memory_space=pl.ANY)
    vmem = pl.BlockSpec(memory_space=pltpu.VMEM)
    dma = pltpu.SemaphoreType.DMA
    hidden, normed = pl.pallas_call(
        kernel,
        out_shape=(
            pltpu.VMEM((D // HEAD, HEAD), BF16),
            pltpu.VMEM((D // HEAD, HEAD), BF16),
        ),
        in_specs=[hbm] * 12,
        out_specs=(vmem, vmem),
        scratch_shapes=[
            pltpu.VMEM((1, HQ * HEAD), BF16),
            pltpu.VMEM((1, KVH * HEAD), BF16),
            pltpu.VMEM((1, KVH * HEAD), BF16),
            pltpu.VMEM((1, D), BF16),
            pltpu.VMEM((D,), BF16),
            pltpu.VMEM((BLOCK, KVH * HEAD), BF16),
            pltpu.VMEM((BLOCK, KVH * HEAD), BF16),
            pltpu.VMEM((BLOCK, HALF_COLS), BF16),
            pltpu.VMEM((BLOCK, HALF_COLS), BF16),
            pltpu.VMEM((8, BLOCK), F32),
            pltpu.VMEM((8, BLOCK), F32),
            pltpu.VMEM((HQ, HEAD), F32),
            pltpu.VMEM((2, HALF_HEADS, HEAD), BF16),
            pltpu.VMEM((N, HALF_HEADS, HEAD), BF16),
            pltpu.VMEM((2, HEAD, HEAD), BF16),
            pltpu.VMEM((HEAD, HEAD), BF16),
            pltpu.VMEM((NB, HALF_KV, RB, HEAD), BF16),
            pltpu.VMEM((NB, HALF_KV, 2, BLOCK), F32),
            pltpu.VMEM((NB, CHIPS, RB, HEAD), BF16),
            pltpu.VMEM((NB, CHIPS, 2, BLOCK), F32),
            pltpu.VMEM((2, 2 * HEAD, HALF_D), BF16),
            pltpu.VMEM((NB, SB, HALF_D // HEAD, HEAD), BF16),
            pltpu.VMEM((CHIPS, 2, HALF_D // HEAD, HEAD), BF16),
            pltpu.VMEM((D // HEAD, HEAD), F32),
            pltpu.VMEM((D // HEAD, HEAD), F32),
            pltpu.SMEM((1,), jnp.int32),
            pltpu.SMEM((1,), jnp.int32),
            pltpu.VMEM((8192, HEAD), F32),
            dma((9,)),
            dma,
            dma((NB,)),
            dma((2,)),
            dma((NB,)),
            dma,
        ],
        compiler_params=pltpu.CompilerParams(collective_id=0, has_side_effects=True),
        name="decode_step",
    )(
        query_new,
        key_new,
        value_new,
        prefix_keys,
        prefix_values,
        sample_suffix_keys,
        sample_suffix_values,
        prefix_len,
        suffix_len,
        residual,
        out_weight,
        norm_gain,
    )
    return hidden.reshape(1, D), normed.reshape(1, D)


def solution(mesh):
    placed = (
        P(("dp", "mp"), None),
        P(("dp", "mp"), None),
        P(("dp", "mp"), None),
        P(("dp", "mp"), None),
        P(("dp", "mp"), None),
        P(("dp", "mp"), None, None),
        P(("dp", "mp"), None, None),
        P("dp"),
        P(("dp", "mp")),
        P(("dp", "mp"), None),
        P("mp", None),
        P(),
    )
    return jax.shard_map(
        local,
        mesh=mesh,
        in_specs=placed,
        out_specs=(P(("dp", "mp"), None), P(("dp", "mp"), None)),
        check_vma=False,
    )
```

```python
import functools

import jax
import jax.numpy as jnp
from jax import lax
from jax.experimental import pallas as pl
from jax.experimental.pallas import tpu as pltpu
from jax.sharding import PartitionSpec as P

HEAD = 128
KVH = 8
HQ = 32
D = 8192
CHIPS = 8
N = 16
HALF_HEADS = 16
HALF_KV = 4
PRE_DEV = 128
SUF = 64
BLOCK = 256
HALF_COLS = HALF_KV * HEAD
HALF_D = D // 2
NEG = -1e30
F32 = jnp.float32
BF16 = jnp.bfloat16
HALF_CHIPS = CHIPS // 2
BATCHES = ((0, 4), (4, 4), (8, 8))
NB = len(BATCHES)
SB = 8
RB = 4 * SB


def nt(a, b):
    return lax.dot_general(a, b, (((1,), (1,)), ((), ())), preferred_element_type=F32)


def nn(a, b):
    return lax.dot_general(a, b, (((1,), (0,)), ((), ())), preferred_element_type=F32)


def kernel(
    q_hbm,
    kn_hbm,
    vn_hbm,
    pk_hbm,
    pv_hbm,
    sk_hbm,
    sv_hbm,
    plen_hbm,
    slen_hbm,
    res_hbm,
    w_hbm,
    gain_hbm,
    hid_ref,
    nrm_ref,
    qv,
    knv,
    vnv,
    resv,
    gainv,
    kfull,
    vfull,
    kpar,
    vpar,
    bias,
    bpar,
    q32,
    qsend,
    qbuf,
    y32,
    ostage,
    sstage,
    obuf,
    sbuf,
    wbuf,
    ysend,
    rbuf,
    res64,
    gain64,
    plen_ref,
    slen_ref,
    bytes_ref,
    loc_sem,
    send_sem,
    qr_sem,
    xr_sem,
    or_sem,
    yr_sem,
):
    me = lax.axis_index("mp")
    z = me // 2
    c = me % 2
    p = 1 - c
    partner = z * 2 + p
    own_half = p
    par_half = c
    my_batch = z // 2 - z // 6

    def at_mp(index):
        return {"mp": index}

    def remote(src, dst, rsem, index):
        return pltpu.make_async_remote_copy(
            src_ref=src,
            dst_ref=dst,
            send_sem=send_sem,
            recv_sem=rsem,
            device_id=at_mp(index),
            device_id_type=pl.DeviceIdType.MESH,
        )

    def wait_total(size, sem):
        wait_bytes(bytes_ref.at[pl.ds(0, size // (4 * HEAD))], sem)

    def wait_bytes(ref, sem):
        pltpu.make_async_copy(ref, ref, sem).wait()

    par_cols = pl.ds(pl.multiple_of(par_half * HALF_COLS, HALF_COLS), HALF_COLS)
    own_d = pl.ds(pl.multiple_of(c * HALF_D, HALF_D), HALF_D)
    par_d = pl.ds(pl.multiple_of(p * HALF_D, HALF_D), HALF_D)
    swaps = [
        remote(kfull.at[:, par_cols], kpar, xr_sem.at[0], partner),
        remote(vfull.at[:, par_cols], vpar, xr_sem.at[0], partner),
        remote(bias, bpar, xr_sem.at[0], partner),
        remote(w_hbm.at[:, par_d], wbuf.at[c], xr_sem.at[1], partner),
    ]
    local = [
        pltpu.make_async_copy(q_hbm, qv, loc_sem.at[0]),
        pltpu.make_async_copy(kn_hbm, knv, loc_sem.at[1]),
        pltpu.make_async_copy(vn_hbm, vnv, loc_sem.at[8]),
        pltpu.make_async_copy(pk_hbm, kfull.at[pl.ds(0, PRE_DEV)], loc_sem.at[2]),
        pltpu.make_async_copy(pv_hbm, vfull.at[pl.ds(0, PRE_DEV)], loc_sem.at[2]),
        pltpu.make_async_copy(sk_hbm.at[0], kfull.at[pl.ds(PRE_DEV, SUF)], loc_sem.at[2]),
        pltpu.make_async_copy(sv_hbm.at[0], vfull.at[pl.ds(PRE_DEV, SUF)], loc_sem.at[2]),
        pltpu.make_async_copy(res_hbm, resv, loc_sem.at[3]),
        pltpu.make_async_copy(gain_hbm, gainv, loc_sem.at[4]),
        pltpu.make_async_copy(w_hbm.at[:, own_d], wbuf.at[c], loc_sem.at[5]),
        pltpu.make_async_copy(plen_hbm, plen_ref, loc_sem.at[6]),
        pltpu.make_async_copy(slen_hbm, slen_ref, loc_sem.at[7]),
    ]

    with jax.named_scope("prep"):
        barrier = pltpu.get_barrier_semaphore()

        for t in range(CHIPS - 1):
            chip = t + 1 + (t - z) // CHIPS
            for half in (0, 1):
                pl.semaphore_signal(
                    barrier,
                    inc=1,
                    device_id=at_mp(chip * 2 + half),
                    device_id_type=pl.DeviceIdType.MESH,
                )
        pl.semaphore_signal(
            barrier, inc=1, device_id=at_mp(partner), device_id_type=pl.DeviceIdType.MESH
        )
        for copy in local:
            copy.start()

        local[10].wait()
        local[11].wait()
        col = lax.broadcasted_iota(jnp.int32, (8, BLOCK), 1)
        valid = (
            ((col < PRE_DEV) & (col + me * PRE_DEV < plen_ref[0]))
            | ((col >= PRE_DEV) & (col < PRE_DEV + SUF) & (col - PRE_DEV < slen_ref[0]))
            | (col == PRE_DEV + SUF)
        )
        bias[...] = jnp.where(valid, 0.0, NEG)

        local[0].wait()
        for h in range(HQ):
            q32[h : h + 1, :] = qv[0:1, h * HEAD : (h + 1) * HEAD].astype(F32)
        qsend[0] = q32[0:HALF_HEADS, :].astype(BF16)
        qsend[1] = q32[HALF_HEADS:HQ, :].astype(BF16)

        pad_rows = BLOCK - PRE_DEV - SUF
        first = lax.broadcasted_iota(jnp.int32, (pad_rows, KVH * HEAD), 0) == 0
        local[1].wait()
        kfull[PRE_DEV + SUF : BLOCK, :] = jnp.where(first, knv[0:1, :].astype(F32), 0.0).astype(
            BF16
        )
        local[2].wait()
        vfull[PRE_DEV + SUF : BLOCK, :] = jnp.where(first, vnv[0:1, :].astype(F32), 0.0).astype(
            BF16
        )

    with jax.named_scope("barrier"):
        pl.semaphore_wait(barrier, N - 1)

    with jax.named_scope("qsend"):

        def send_query(i, carry):
            k = i // 2
            half = i % 2
            step = CHIPS // 2 + ((k + 1) // 2) * (1 - 2 * (k % 2))
            target = ((z + step) % CHIPS) * 2 + 1 - half
            remote(qsend.at[half], qbuf.at[me], qr_sem.at[my_batch], target).start()
            return carry

        lax.fori_loop(0, N - 2, send_query, 0)
        remote(qsend.at[par_half], qbuf.at[me], qr_sem.at[my_batch], partner).start()
        pltpu.make_async_copy(qsend.at[own_half], qbuf.at[me], qr_sem.at[my_batch]).start()

    with jax.named_scope("kvsend"):
        wait_total(2 * 2 * (PRE_DEV + SUF) * KVH * HEAD, loc_sem.at[2])
        for copy in swaps:
            copy.start()

    with jax.named_scope("resgain"):
        local[7].wait()
        local[8].wait()
        for r in range(D // HEAD):
            res64[r : r + 1, :] = resv[0:1, r * HEAD : (r + 1) * HEAD].astype(F32)
            gain64[r, :] = gainv[r * HEAD : (r + 1) * HEAD].astype(F32)

    with jax.named_scope("kvwait"):
        wait_total(2 * 2 * BLOCK * HALF_COLS + 4 * 8 * BLOCK, xr_sem.at[0])

    scale = HEAD ** (-0.5)

    def diagonal(ns):
        rows = lax.broadcasted_iota(jnp.int32, (4 * ns, 32 * ns), 0)
        cols = lax.broadcasted_iota(jnp.int32, (4 * ns, 32 * ns), 1)
        return cols % (4 * ns) == rows

    def regrouped(ns):
        rows = lax.broadcasted_iota(jnp.int32, (4 * ns, 32 * ns), 0)
        cols = lax.broadcasted_iota(jnp.int32, (4 * ns, 32 * ns), 1)
        return cols % (4 * ns) == (rows % ns) * 4 + rows // ns

    def sums_bytes(ns):
        return 2 * 4 * ns * HEAD + 4 * 2 * 32 * ns

    def attend(b):
        start, ns = BATCHES[b]
        rb = 4 * ns
        with jax.named_scope("qwait%d" % b):
            wait_bytes(qbuf.at[pl.ds(start, ns)], qr_sem.at[b])
        with jax.named_scope("attn%d" % b):
            arrived = qbuf[start : start + ns].astype(F32)
            queries = [
                jnp.concatenate([arrived[i, 4 * j : 4 * j + 4, :] for i in range(ns)], axis=0)
                for j in range(HALF_KV)
            ]
            sample = lax.broadcasted_iota(jnp.int32, (rb, BLOCK), 0) // 4 + start
            shared = lax.broadcasted_iota(jnp.int32, (rb, BLOCK), 1) < PRE_DEV
            bias_own = jnp.where(shared | (sample == me), bias[0:1, :], NEG)
            bias_par = jnp.where(shared | (sample == partner), bpar[0:1, :], NEG)
            scores = []
            for j in range(HALF_KV):
                qj = queries[j].astype(BF16)
                at_own = pl.ds(pl.multiple_of(own_half * HALF_COLS + j * HEAD, HEAD), HEAD)
                scores.append(
                    (
                        nt(qj, kfull[:, at_own]) * scale + bias_own,
                        nt(qj, kpar[:, j * HEAD : (j + 1) * HEAD]) * scale + bias_par,
                    )
                )
            tops = [jnp.max(jnp.maximum(x, y), axis=1, keepdims=True) for x, y in scores]
            weights = [(jnp.exp(x - t), jnp.exp(y - t)) for (x, y), t in zip(scores, tops)]
            totals = [jnp.sum(x + y, axis=1, keepdims=True) for x, y in weights]
            for j in range(HALF_KV):
                at_own = pl.ds(pl.multiple_of(own_half * HALF_COLS + j * HEAD, HEAD), HEAD)
                w_own, w_par = weights[j]
                out = nn(w_own.astype(BF16), vfull[:, at_own]) + nn(
                    w_par.astype(BF16), vpar[:, j * HEAD : (j + 1) * HEAD]
                )
                ostage[b, j, 0:rb, :] = out.astype(BF16)
            for j in range(HALF_KV):
                for i, stat in enumerate((tops[j], totals[j])):
                    sstage[b, j, i : i + 1, 0 : 8 * rb] = jnp.sum(
                        jnp.where(diagonal(ns), stat, 0.0), axis=0, keepdims=True
                    )
        with jax.named_scope("osend%d" % b):
            for i in (1, 2, 3, 0):
                j = (z + i) % HALF_CHIPS
                for half in range(2):
                    target = (HALF_CHIPS * own_half + j) * 2 + half
                    pairs = (
                        (ostage.at[b, j, pl.ds(0, rb)], obuf.at[b, z, pl.ds(0, rb)]),
                        (
                            sstage.at[b, j, :, pl.ds(0, 8 * rb)],
                            sbuf.at[b, z, :, pl.ds(0, 8 * rb)],
                        ),
                    )
                    if i:
                        for src, dst in pairs:
                            remote(src, dst, or_sem.at[b], target).start()
                        continue

                    @pl.when(target != me)
                    def _():
                        for src, dst in pairs:
                            remote(src, dst, or_sem.at[b], target).start()

                    @pl.when(target == me)
                    def _():
                        for src, dst in pairs:
                            pltpu.make_async_copy(src, dst, or_sem.at[b]).start()

    def project(b):
        start, ns = BATCHES[b]
        rb = 4 * ns
        with jax.named_scope("owait%d" % b):
            wait_total(CHIPS * sums_bytes(ns), or_sem.at[b])
        with jax.named_scope("combine%d" % b):
            stats = sbuf[b, :, :, 0 : 8 * rb]
            group = lax.broadcasted_iota(jnp.int32, (1, 8 * rb), 1) // rb
            most = stats[0, 0:1, :]
            for src_z in range(1, CHIPS):
                most = jnp.maximum(most, stats[src_z, 0:1, :])
            summed = jnp.zeros((1, 8 * rb), F32)
            factor = jnp.zeros((1, 8 * rb), F32)
            for src_z in range(CHIPS):
                f = jnp.exp(stats[src_z, 0:1, :] - most)
                summed = summed + f * stats[src_z, 1:2, :]
                factor = jnp.where(group == src_z, f, factor)
            mix = jnp.where(regrouped(ns), factor / summed, 0.0)
            high = mix.astype(BF16)
            low = (mix - high.astype(F32)).astype(BF16)
            parts = obuf[b, :, 0:rb, :].reshape(CHIPS * rb, HEAD)
            attn = nn(high, parts) + nn(low, parts)
            attn = jnp.concatenate([attn[ns * h : ns * (h + 1), :] for h in range(4)], axis=1)
            if ns < SB:
                attn = jnp.concatenate([attn, jnp.zeros((SB - ns, 4 * HEAD), F32)], axis=0)
            attn = attn.astype(BF16)
        if b == 0:
            with jax.named_scope("waitw"):
                local[9].wait()
                swaps[3].wait_recv()
        with jax.named_scope("proj%d" % b):
            y = nn(attn[:, 0 : 2 * HEAD], wbuf[0]) + nn(attn[:, 2 * HEAD : 4 * HEAD], wbuf[1])
            for i in range(HALF_D // HEAD):
                y32[SB * i : SB * (i + 1), :] = y[:, HEAD * i : HEAD * (i + 1)]
            for t in range(ns):
                ysend[b, t] = y32[pl.ds(t, HALF_D // HEAD, stride=SB), :].astype(BF16)
        with jax.named_scope("ysend%d" % b):

            def send_projection(i, carry):
                t = i + 1 - 2 * (i % 2)
                target = start + t

                @pl.when(target != me)
                def _():
                    remote(ysend.at[b, t], rbuf.at[z, c], yr_sem, target).start()

                @pl.when(target == me)
                def _():
                    pltpu.make_async_copy(ysend.at[b, t], rbuf.at[z, c], yr_sem).start()

                return carry

            lax.fori_loop(0, ns, send_projection, 0)

    for b in (0, 2, 1):
        attend(b)
    project(0)

    @pl.when(my_batch < 2)
    def _():
        project(2)
        project(1)

    @pl.when(my_batch == 2)
    def _():
        project(1)
        project(2)


    with jax.named_scope("ywait"):
        wait_bytes(rbuf, yr_sem)
    with jax.named_scope("final"):
        stream = res64[...] + jnp.sum(rbuf[...].astype(F32), axis=0).reshape(D // HEAD, HEAD)
        meansq = jnp.sum(stream * stream, keepdims=True) * (1.0 / D)
        normed = stream * lax.rsqrt(meansq + 1e-05) * gain64[...]
        hid_ref[...] = stream.astype(BF16)
        nrm_ref[...] = normed.astype(BF16)
    with jax.named_scope("sendwait"):
        sent = (N - 1) * 2 * HALF_HEADS * HEAD
        sent += 2 * 2 * BLOCK * HALF_COLS + 4 * 8 * BLOCK + 2 * 2 * HEAD * HALF_D
        sent += sum(2 * HALF_CHIPS * sums_bytes(ns) for _, ns in BATCHES)
        sent += (N - 1) * 2 * HALF_D
        own_chip = z // HALF_CHIPS == own_half

        @pl.when(own_chip)
        def _():
            wait_total(sent - sum(sums_bytes(ns) for _, ns in BATCHES), send_sem)

        @pl.when(jnp.logical_not(own_chip))
        def _():
            wait_total(sent, send_sem)


def local(
    query_new,
    key_new,
    value_new,
    prefix_keys,
    prefix_values,
    sample_suffix_keys,
    sample_suffix_values,
    prefix_len,
    suffix_len,
    residual,
    out_weight,
    norm_gain,
):
    hbm = pl.BlockSpec(memory_space=pl.ANY)
    vmem = pl.BlockSpec(memory_space=pltpu.VMEM)
    dma = pltpu.SemaphoreType.DMA
    hidden, normed = pl.pallas_call(
        kernel,
        out_shape=(
            pltpu.VMEM((D // HEAD, HEAD), BF16),
            pltpu.VMEM((D // HEAD, HEAD), BF16),
        ),
        in_specs=[hbm] * 12,
        out_specs=(vmem, vmem),
        scratch_shapes=[
            pltpu.VMEM((1, HQ * HEAD), BF16),
            pltpu.VMEM((1, KVH * HEAD), BF16),
            pltpu.VMEM((1, KVH * HEAD), BF16),
            pltpu.VMEM((1, D), BF16),
            pltpu.VMEM((D,), BF16),
            pltpu.VMEM((BLOCK, KVH * HEAD), BF16),
            pltpu.VMEM((BLOCK, KVH * HEAD), BF16),
            pltpu.VMEM((BLOCK, HALF_COLS), BF16),
            pltpu.VMEM((BLOCK, HALF_COLS), BF16),
            pltpu.VMEM((8, BLOCK), F32),
            pltpu.VMEM((8, BLOCK), F32),
            pltpu.VMEM((HQ, HEAD), F32),
            pltpu.VMEM((2, HALF_HEADS, HEAD), BF16),
            pltpu.VMEM((N, HALF_HEADS, HEAD), BF16),
            pltpu.VMEM((SB * HALF_D // HEAD, HEAD), F32),
            pltpu.VMEM((NB, HALF_KV, RB, HEAD), BF16),
            pltpu.VMEM((NB, HALF_KV, 2, BLOCK), F32),
            pltpu.VMEM((NB, CHIPS, RB, HEAD), BF16),
            pltpu.VMEM((NB, CHIPS, 2, BLOCK), F32),
            pltpu.VMEM((2, 2 * HEAD, HALF_D), BF16),
            pltpu.VMEM((NB, SB, HALF_D // HEAD, HEAD), BF16),
            pltpu.VMEM((CHIPS, 2, HALF_D // HEAD, HEAD), BF16),
            pltpu.VMEM((D // HEAD, HEAD), F32),
            pltpu.VMEM((D // HEAD, HEAD), F32),
            pltpu.SMEM((1,), jnp.int32),
            pltpu.SMEM((1,), jnp.int32),
            pltpu.VMEM((8192, HEAD), F32),
            dma((9,)),
            dma,
            dma((NB,)),
            dma((2,)),
            dma((NB,)),
            dma,
        ],
        compiler_params=pltpu.CompilerParams(collective_id=0, has_side_effects=True),
        name="decode_step",
    )(
        query_new,
        key_new,
        value_new,
        prefix_keys,
        prefix_values,
        sample_suffix_keys,
        sample_suffix_values,
        prefix_len,
        suffix_len,
        residual,
        out_weight,
        norm_gain,
    )
    return hidden.reshape(1, D), normed.reshape(1, D)


def solution(mesh):
    placed = (
        P(("dp", "mp"), None),
        P(("dp", "mp"), None),
        P(("dp", "mp"), None),
        P(("dp", "mp"), None),
        P(("dp", "mp"), None),
        P(("dp", "mp"), None, None),
        P(("dp", "mp"), None, None),
        P("dp"),
        P(("dp", "mp")),
        P(("dp", "mp"), None),
        P("mp", None),
        P(),
    )
    return jax.shard_map(
        local,
        mesh=mesh,
        in_specs=placed,
        out_specs=(P(("dp", "mp"), None), P(("dp", "mp"), None)),
        check_vma=False,
    )
```

```python
import functools

import jax
import jax.numpy as jnp
from jax import lax
from jax.experimental import pallas as pl
from jax.experimental.pallas import tpu as pltpu
from jax.sharding import PartitionSpec as P

HEAD = 128
KVH = 8
HQ = 32
D = 8192
CHIPS = 8
N = 16
HALF_HEADS = 16
HALF_KV = 4
PRE_DEV = 128
SUF = 64
BLOCK = 256
HALF_COLS = HALF_KV * HEAD
HALF_D = D // 2
NEG = -1e30
F32 = jnp.float32
BF16 = jnp.bfloat16
HALF_CHIPS = CHIPS // 2
BATCHES = ((0, 4), (4, 4), (8, 8))
NB = len(BATCHES)
SB = 8
RB = 4 * SB


def nt(a, b):
    return lax.dot_general(a, b, (((1,), (1,)), ((), ())), preferred_element_type=F32)


def nn(a, b):
    return lax.dot_general(a, b, (((1,), (0,)), ((), ())), preferred_element_type=F32)


def kernel(
    q_hbm,
    kn_hbm,
    vn_hbm,
    pk_hbm,
    pv_hbm,
    sk_hbm,
    sv_hbm,
    plen_hbm,
    slen_hbm,
    res_hbm,
    w_hbm,
    gain_hbm,
    hid_ref,
    nrm_ref,
    qv,
    knv,
    vnv,
    resv,
    gainv,
    kfull,
    vfull,
    kpar,
    vpar,
    bias,
    bpar,
    q32,
    qsend,
    qbuf,
    y32,
    ostage,
    sstage,
    obuf,
    sbuf,
    wbuf,
    ysend,
    rbuf,
    res64,
    gain64,
    plen_ref,
    slen_ref,
    bytes_ref,
    loc_sem,
    send_sem,
    qr_sem,
    xr_sem,
    or_sem,
    yr_sem,
):
    me = lax.axis_index("mp")
    z = me // 2
    c = me % 2
    p = 1 - c
    partner = z * 2 + p
    own_half = p
    par_half = c
    my_batch = z // 2 - z // 6

    def at_mp(index):
        return {"mp": index}

    def remote(src, dst, rsem, index):
        return pltpu.make_async_remote_copy(
            src_ref=src,
            dst_ref=dst,
            send_sem=send_sem,
            recv_sem=rsem,
            device_id=at_mp(index),
            device_id_type=pl.DeviceIdType.MESH,
        )

    def wait_total(size, sem):
        wait_bytes(bytes_ref.at[pl.ds(0, size // (4 * HEAD))], sem)

    def wait_bytes(ref, sem):
        pltpu.make_async_copy(ref, ref, sem).wait()

    par_cols = pl.ds(pl.multiple_of(par_half * HALF_COLS, HALF_COLS), HALF_COLS)
    own_d = pl.ds(pl.multiple_of(c * HALF_D, HALF_D), HALF_D)
    par_d = pl.ds(pl.multiple_of(p * HALF_D, HALF_D), HALF_D)
    swaps = [
        remote(kfull.at[:, par_cols], kpar, xr_sem.at[0], partner),
        remote(vfull.at[:, par_cols], vpar, xr_sem.at[0], partner),
        remote(bias, bpar, xr_sem.at[0], partner),
        remote(w_hbm.at[:, par_d], wbuf.at[c], xr_sem.at[1], partner),
    ]
    local = [
        pltpu.make_async_copy(q_hbm, qv, loc_sem.at[0]),
        pltpu.make_async_copy(kn_hbm, knv, loc_sem.at[1]),
        pltpu.make_async_copy(vn_hbm, vnv, loc_sem.at[8]),
        pltpu.make_async_copy(pk_hbm, kfull.at[pl.ds(0, PRE_DEV)], loc_sem.at[2]),
        pltpu.make_async_copy(pv_hbm, vfull.at[pl.ds(0, PRE_DEV)], loc_sem.at[2]),
        pltpu.make_async_copy(sk_hbm.at[0], kfull.at[pl.ds(PRE_DEV, SUF)], loc_sem.at[2]),
        pltpu.make_async_copy(sv_hbm.at[0], vfull.at[pl.ds(PRE_DEV, SUF)], loc_sem.at[2]),
        pltpu.make_async_copy(res_hbm, resv, loc_sem.at[3]),
        pltpu.make_async_copy(gain_hbm, gainv, loc_sem.at[4]),
        pltpu.make_async_copy(w_hbm.at[:, own_d], wbuf.at[c], loc_sem.at[5]),
        pltpu.make_async_copy(plen_hbm, plen_ref, loc_sem.at[6]),
        pltpu.make_async_copy(slen_hbm, slen_ref, loc_sem.at[7]),
    ]

    with jax.named_scope("prep"):
        barrier = pltpu.get_barrier_semaphore()

        for t in range(CHIPS - 1):
            chip = t + 1 + (t - z) // CHIPS
            for half in (0, 1):
                pl.semaphore_signal(
                    barrier,
                    inc=1,
                    device_id=at_mp(chip * 2 + half),
                    device_id_type=pl.DeviceIdType.MESH,
                )
        pl.semaphore_signal(
            barrier, inc=1, device_id=at_mp(partner), device_id_type=pl.DeviceIdType.MESH
        )
        for copy in local:
            copy.start()

        local[10].wait()
        local[11].wait()
        col = lax.broadcasted_iota(jnp.int32, (8, BLOCK), 1)
        valid = (
            ((col < PRE_DEV) & (col + me * PRE_DEV < plen_ref[0]))
            | ((col >= PRE_DEV) & (col < PRE_DEV + SUF) & (col - PRE_DEV < slen_ref[0]))
            | (col == PRE_DEV + SUF)
        )
        bias[...] = jnp.where(valid, 0.0, NEG)

        local[0].wait()
        for h in range(HQ):
            q32[h : h + 1, :] = qv[0:1, h * HEAD : (h + 1) * HEAD].astype(F32)
        qsend[0] = q32[0:HALF_HEADS, :].astype(BF16)
        qsend[1] = q32[HALF_HEADS:HQ, :].astype(BF16)

        pad_rows = BLOCK - PRE_DEV - SUF
        first = lax.broadcasted_iota(jnp.int32, (pad_rows, KVH * HEAD), 0) == 0
        local[1].wait()
        kfull[PRE_DEV + SUF : BLOCK, :] = jnp.where(first, knv[0:1, :].astype(F32), 0.0).astype(
            BF16
        )
        local[2].wait()
        vfull[PRE_DEV + SUF : BLOCK, :] = jnp.where(first, vnv[0:1, :].astype(F32), 0.0).astype(
            BF16
        )

    with jax.named_scope("barrier"):
        pl.semaphore_wait(barrier, N - 1)

    with jax.named_scope("qsend"):

        def send_query(i, carry):
            k = i // 2
            half = i % 2
            step = CHIPS // 2 + ((k + 1) // 2) * (1 - 2 * (k % 2))
            target = ((z + step) % CHIPS) * 2 + 1 - half
            remote(qsend.at[half], qbuf.at[me], qr_sem.at[my_batch], target).start()
            return carry

        lax.fori_loop(0, N - 2, send_query, 0)
        remote(qsend.at[par_half], qbuf.at[me], qr_sem.at[my_batch], partner).start()
        pltpu.make_async_copy(qsend.at[own_half], qbuf.at[me], qr_sem.at[my_batch]).start()

    with jax.named_scope("kvsend"):
        wait_total(2 * 2 * (PRE_DEV + SUF) * KVH * HEAD, loc_sem.at[2])
        for copy in swaps:
            copy.start()

    with jax.named_scope("resgain"):
        local[7].wait()
        local[8].wait()
        for r in range(D // HEAD):
            res64[r : r + 1, :] = resv[0:1, r * HEAD : (r + 1) * HEAD].astype(F32)
            gain64[r, :] = gainv[r * HEAD : (r + 1) * HEAD].astype(F32)

    with jax.named_scope("kvwait"):
        wait_total(2 * 2 * BLOCK * HALF_COLS + 4 * 8 * BLOCK, xr_sem.at[0])

    scale = HEAD ** (-0.5)

    def diagonal(ns):
        rows = lax.broadcasted_iota(jnp.int32, (4 * ns, 32 * ns), 0)
        cols = lax.broadcasted_iota(jnp.int32, (4 * ns, 32 * ns), 1)
        return cols % (4 * ns) == rows

    def regrouped(ns):
        rows = lax.broadcasted_iota(jnp.int32, (4 * ns, 32 * ns), 0)
        cols = lax.broadcasted_iota(jnp.int32, (4 * ns, 32 * ns), 1)
        return cols % (4 * ns) == (rows % ns) * 4 + rows // ns

    def sums_bytes(ns):
        return 2 * 4 * ns * HEAD + 4 * 2 * 32 * ns

    def attend(b):
        start, ns = BATCHES[b]
        rb = 4 * ns
        with jax.named_scope("qwait%d" % b):
            wait_bytes(qbuf.at[pl.ds(start, ns)], qr_sem.at[b])
        with jax.named_scope("attn%d" % b):
            arrived = qbuf[start : start + ns].astype(F32)
            queries = [
                jnp.concatenate([arrived[i, 4 * j : 4 * j + 4, :] for i in range(ns)], axis=0)
                for j in range(HALF_KV)
            ]
            sample = lax.broadcasted_iota(jnp.int32, (rb, BLOCK), 0) // 4 + start
            shared = lax.broadcasted_iota(jnp.int32, (rb, BLOCK), 1) < PRE_DEV
            bias_own = jnp.where(shared | (sample == me), bias[0:1, :], NEG)
            bias_par = jnp.where(shared | (sample == partner), bpar[0:1, :], NEG)
            scores = []
            for j in range(HALF_KV):
                qj = queries[j].astype(BF16)
                at_own = pl.ds(pl.multiple_of(own_half * HALF_COLS + j * HEAD, HEAD), HEAD)
                scores.append(
                    (
                        nt(qj, kfull[:, at_own]) * scale + bias_own,
                        nt(qj, kpar[:, j * HEAD : (j + 1) * HEAD]) * scale + bias_par,
                    )
                )
            tops = [jnp.max(jnp.maximum(x, y), axis=1, keepdims=True) for x, y in scores]
            weights = [(jnp.exp(x - t), jnp.exp(y - t)) for (x, y), t in zip(scores, tops)]
            totals = [jnp.sum(x + y, axis=1, keepdims=True) for x, y in weights]
            for j in range(HALF_KV):
                at_own = pl.ds(pl.multiple_of(own_half * HALF_COLS + j * HEAD, HEAD), HEAD)
                w_own, w_par = weights[j]
                out = nn(w_own.astype(BF16), vfull[:, at_own]) + nn(
                    w_par.astype(BF16), vpar[:, j * HEAD : (j + 1) * HEAD]
                )
                ostage[b, j, 0:rb, :] = out.astype(BF16)
            for j in range(HALF_KV):
                for i, stat in enumerate((tops[j], totals[j])):
                    sstage[b, j, i : i + 1, 0 : 8 * rb] = jnp.sum(
                        jnp.where(diagonal(ns), stat, 0.0), axis=0, keepdims=True
                    )

    def send_sums(b):
        rb = 4 * BATCHES[b][1]
        with jax.named_scope("osend%d" % b):
            for i in (1, 2, 3, 0):
                j = (z + i) % HALF_CHIPS
                for half in range(2):
                    target = (HALF_CHIPS * own_half + j) * 2 + half
                    pairs = (
                        (ostage.at[b, j, pl.ds(0, rb)], obuf.at[b, z, pl.ds(0, rb)]),
                        (
                            sstage.at[b, j, :, pl.ds(0, 8 * rb)],
                            sbuf.at[b, z, :, pl.ds(0, 8 * rb)],
                        ),
                    )
                    if i:
                        for src, dst in pairs:
                            remote(src, dst, or_sem.at[b], target).start()
                        continue

                    @pl.when(target != me)
                    def _():
                        for src, dst in pairs:
                            remote(src, dst, or_sem.at[b], target).start()

                    @pl.when(target == me)
                    def _():
                        for src, dst in pairs:
                            pltpu.make_async_copy(src, dst, or_sem.at[b]).start()

    def send_projections(b, low, high):
        start, ns = BATCHES[b]

        def send_projection(i, carry):
            t = i + 1 - 2 * (i % 2)
            target = start + t

            @pl.when(target != me)
            def _():
                remote(ysend.at[b, t], rbuf.at[z, c], yr_sem, target).start()

            @pl.when(target == me)
            def _():
                pltpu.make_async_copy(ysend.at[b, t], rbuf.at[z, c], yr_sem).start()

            return carry

        lax.fori_loop(low, high, send_projection, 0)

    def project(b, after_first=False):
        start, ns = BATCHES[b]
        rb = 4 * ns
        with jax.named_scope("owait%d" % b):
            wait_total(CHIPS * sums_bytes(ns), or_sem.at[b])
        with jax.named_scope("combine%d" % b):
            stats = sbuf[b, :, :, 0 : 8 * rb]
            group = lax.broadcasted_iota(jnp.int32, (1, 8 * rb), 1) // rb
            most = stats[0, 0:1, :]
            for src_z in range(1, CHIPS):
                most = jnp.maximum(most, stats[src_z, 0:1, :])
            summed = jnp.zeros((1, 8 * rb), F32)
            factor = jnp.zeros((1, 8 * rb), F32)
            for src_z in range(CHIPS):
                f = jnp.exp(stats[src_z, 0:1, :] - most)
                summed = summed + f * stats[src_z, 1:2, :]
                factor = jnp.where(group == src_z, f, factor)
            mix = jnp.where(regrouped(ns), factor / summed, 0.0)
            high = mix.astype(BF16)
            low = (mix - high.astype(F32)).astype(BF16)
            parts = obuf[b, :, 0:rb, :].reshape(CHIPS * rb, HEAD)
            attn = nn(high, parts) + nn(low, parts)
            attn = jnp.concatenate([attn[ns * h : ns * (h + 1), :] for h in range(4)], axis=1)
            if ns < SB:
                attn = jnp.concatenate([attn, jnp.zeros((SB - ns, 4 * HEAD), F32)], axis=0)
            attn = attn.astype(BF16)
        if after_first:
            send_projections(0, 2, BATCHES[0][1])
        if b == 0:
            with jax.named_scope("waitw"):
                local[9].wait()
                swaps[3].wait_recv()
        with jax.named_scope("proj%d" % b):
            y = nn(attn[:, 0 : 2 * HEAD], wbuf[0]) + nn(attn[:, 2 * HEAD : 4 * HEAD], wbuf[1])
            for i in range(HALF_D // HEAD):
                y32[SB * i : SB * (i + 1), :] = y[:, HEAD * i : HEAD * (i + 1)]
            for t in range(ns):
                ysend[b, t] = y32[pl.ds(t, HALF_D // HEAD, stride=SB), :].astype(BF16)
        with jax.named_scope("ysend%d" % b):

            send_projections(b, 0, 2 if b == 0 else ns)

    attend(0)
    send_sums(0)
    attend(2)
    attend(1)
    send_sums(1)
    send_sums(2)
    project(0)
    project(1, True)
    project(2)

    with jax.named_scope("ywait"):
        wait_bytes(rbuf, yr_sem)
    with jax.named_scope("final"):
        stream = res64[...] + jnp.sum(rbuf[...].astype(F32), axis=0).reshape(D // HEAD, HEAD)
        meansq = jnp.sum(stream * stream, keepdims=True) * (1.0 / D)
        normed = stream * lax.rsqrt(meansq + 1e-05) * gain64[...]
        hid_ref[...] = stream.astype(BF16)
        nrm_ref[...] = normed.astype(BF16)
    with jax.named_scope("sendwait"):
        sent = (N - 1) * 2 * HALF_HEADS * HEAD
        sent += 2 * 2 * BLOCK * HALF_COLS + 4 * 8 * BLOCK + 2 * 2 * HEAD * HALF_D
        sent += sum(2 * HALF_CHIPS * sums_bytes(ns) for _, ns in BATCHES)
        sent += (N - 1) * 2 * HALF_D
        own_chip = z // HALF_CHIPS == own_half

        @pl.when(own_chip)
        def _():
            wait_total(sent - sum(sums_bytes(ns) for _, ns in BATCHES), send_sem)

        @pl.when(jnp.logical_not(own_chip))
        def _():
            wait_total(sent, send_sem)


def local(
    query_new,
    key_new,
    value_new,
    prefix_keys,
    prefix_values,
    sample_suffix_keys,
    sample_suffix_values,
    prefix_len,
    suffix_len,
    residual,
    out_weight,
    norm_gain,
):
    hbm = pl.BlockSpec(memory_space=pl.ANY)
    vmem = pl.BlockSpec(memory_space=pltpu.VMEM)
    dma = pltpu.SemaphoreType.DMA
    hidden, normed = pl.pallas_call(
        kernel,
        out_shape=(
            pltpu.VMEM((D // HEAD, HEAD), BF16),
            pltpu.VMEM((D // HEAD, HEAD), BF16),
        ),
        in_specs=[hbm] * 12,
        out_specs=(vmem, vmem),
        scratch_shapes=[
            pltpu.VMEM((1, HQ * HEAD), BF16),
            pltpu.VMEM((1, KVH * HEAD), BF16),
            pltpu.VMEM((1, KVH * HEAD), BF16),
            pltpu.VMEM((1, D), BF16),
            pltpu.VMEM((D,), BF16),
            pltpu.VMEM((BLOCK, KVH * HEAD), BF16),
            pltpu.VMEM((BLOCK, KVH * HEAD), BF16),
            pltpu.VMEM((BLOCK, HALF_COLS), BF16),
            pltpu.VMEM((BLOCK, HALF_COLS), BF16),
            pltpu.VMEM((8, BLOCK), F32),
            pltpu.VMEM((8, BLOCK), F32),
            pltpu.VMEM((HQ, HEAD), F32),
            pltpu.VMEM((2, HALF_HEADS, HEAD), BF16),
            pltpu.VMEM((N, HALF_HEADS, HEAD), BF16),
            pltpu.VMEM((SB * HALF_D // HEAD, HEAD), F32),
            pltpu.VMEM((NB, HALF_KV, RB, HEAD), BF16),
            pltpu.VMEM((NB, HALF_KV, 2, BLOCK), F32),
            pltpu.VMEM((NB, CHIPS, RB, HEAD), BF16),
            pltpu.VMEM((NB, CHIPS, 2, BLOCK), F32),
            pltpu.VMEM((2, 2 * HEAD, HALF_D), BF16),
            pltpu.VMEM((NB, SB, HALF_D // HEAD, HEAD), BF16),
            pltpu.VMEM((CHIPS, 2, HALF_D // HEAD, HEAD), BF16),
            pltpu.VMEM((D // HEAD, HEAD), F32),
            pltpu.VMEM((D // HEAD, HEAD), F32),
            pltpu.SMEM((1,), jnp.int32),
            pltpu.SMEM((1,), jnp.int32),
            pltpu.VMEM((8192, HEAD), F32),
            dma((9,)),
            dma,
            dma((NB,)),
            dma((2,)),
            dma((NB,)),
            dma,
        ],
        compiler_params=pltpu.CompilerParams(collective_id=0, has_side_effects=True),
        name="decode_step",
    )(
        query_new,
        key_new,
        value_new,
        prefix_keys,
        prefix_values,
        sample_suffix_keys,
        sample_suffix_values,
        prefix_len,
        suffix_len,
        residual,
        out_weight,
        norm_gain,
    )
    return hidden.reshape(1, D), normed.reshape(1, D)


def solution(mesh):
    placed = (
        P(("dp", "mp"), None),
        P(("dp", "mp"), None),
        P(("dp", "mp"), None),
        P(("dp", "mp"), None),
        P(("dp", "mp"), None),
        P(("dp", "mp"), None, None),
        P(("dp", "mp"), None, None),
        P("dp"),
        P(("dp", "mp")),
        P(("dp", "mp"), None),
        P("mp", None),
        P(),
    )
    return jax.shard_map(
        local,
        mesh=mesh,
        in_specs=placed,
        out_specs=(P(("dp", "mp"), None), P(("dp", "mp"), None)),
        check_vma=False,
    )
```
